32 devices in a mesh: aa: 8 (over y, x, core), ba: 4 (over z).
Axes of the slice: x: 2, y: 2, z: 4, core: 2. Of those that a mesh axis runs over, the one named last changes fastest.
Arguments:
- cotangent: bfloat16 [1, 20, 64, 64, 2048], P(None, None, 'aa', 'ba'), may hold values from -6 to 6
- pre_activations: bfloat16 [2, 1, 20, 64, 64, 2048], P(None, None, None, 'aa', 'ba'), may hold values from -6 to 6
- spectral_weights: bfloat16 [2, 2, 20, 20, 24, 6912], P(None, None, None, None, 'ba', 'aa'), may hold values from -6 to 6
- skip_weights: bfloat16 [2, 20, 20], replicated, may hold values from -1.25 to 1.25
- lift_weights: float32 [20], replicated, may hold values from -1.25 to 1.25
Outputs:
- perm_grad: float32 [1, 64, 64, 2048], P(None, 'aa', 'ba')
The draws below stay inside these ranges and needn't reach their ends.
All inputs are finite; a program needn't handle non-finite values.
Results may differ from the reference program's by a relative error of at most 0.023.
Values may be sent and summed in bfloat16 or wider, within the bound.
A program may use at most 256 MiB of HBM per device.

```python
import math
import jax
import jax.numpy as jnp
from jax import lax

C = 20
NX = 64
NY = 64
NZ = 64
NT = 32
KX = 24
KY = 24
KZ = 24
KT = 12
LAYERS = 2
B = 1


def level_of(key, extent, cuts, smallest, top_value):
    factor_of = 1.0
    for dim, blocks in cuts:
        steps = jax.random.uniform(jax.random.fold_in(jax.random.fold_in(key, 6), dim), (blocks,), jnp.float32, smallest / len(cuts), top_value / len(cuts))
        factor_of = factor_of * jnp.repeat(jnp.exp(steps), extent[dim] // blocks).reshape((-1,) + (1,) * (len(extent) - 1 - dim))
    return factor_of


def normal_values(key, dims, deviation, reach, pieces=(), kind=jnp.bfloat16):
    entries = deviation * jax.random.normal(key, dims, jnp.float32)
    if pieces:
        entries = entries * level_of(key, dims, pieces, -0.22, 0.18)
    return jnp.clip(entries, -reach, reach).astype(kind)


def setup_inputs(seed: int = 0) -> dict:
    key_of = jax.random.split(jax.random.key(seed), 6)
    return {
        "cotangent": normal_values(key_of[0], (B, C, NX, NY, NZ * NT), 1.0, 6.0, ((2, 8), (3, 4))),
        "pre_activations": normal_values(key_of[1], (LAYERS, B, C, NX, NY, NZ * NT), 1.0, 6.0, ((3, 8), (4, 4))),
        "spectral_weights": normal_values(key_of[2], (LAYERS, 2, C, C, KX, KZ * KT * KY), ((NX * NY * NZ * NT) ** 0.5 * (KX * KY * KZ * KT * C) ** -0.5), 6.0, ((4, 4), (5, 8))),
        "skip_weights": normal_values(key_of[3], (LAYERS, C, C), C ** -0.5, 1.25),
        "lift_weights": normal_values(key_of[4], (C,), C ** -0.5, 1.25, (), jnp.float32),
    }


def gelu_slope(values):
    normal_cdf = 0.5 * (1.0 + lax.erf(values / math.sqrt(2.0)))
    density = jnp.exp(-0.5 * values * values) / math.sqrt(2.0 * math.pi)
    return normal_cdf + values * density

def round_complex(values):
    real_part = lax.optimization_barrier(values.real.astype(jnp.bfloat16)).astype(jnp.float32)
    imag_part = lax.optimization_barrier(values.imag.astype(jnp.bfloat16)).astype(jnp.float32)
    return lax.complex(real_part, imag_part)

def kept_index(total_count, length):
    return jnp.concatenate([jnp.arange(total_count // 2, dtype=jnp.int32), jnp.arange(length - total_count // 2, length, dtype=jnp.int32)])

def forward_field(field):
    values = field.astype(jnp.float32).reshape(NX, NY, NZ, NT)
    spectrum = jnp.fft.fft2(values, axes=(2, 3))
    spectrum = jnp.take(spectrum, kept_index(KZ, NZ), axis=2)
    spectrum = round_complex(spectrum[:, :, :, :KT])
    spectrum = round_complex(jnp.take(jnp.fft.fft(spectrum, axis=0), kept_index(KX, NX), axis=0))
    spectrum = round_complex(jnp.take(jnp.fft.fft(spectrum, axis=1), kept_index(KY, NY), axis=1))
    return spectrum

def inverse_field(mode_values, rounded):
    gridded = jnp.zeros((KX, NY, KZ, KT), mode_values.dtype).at[:, kept_index(KY, NY)].set(mode_values)
    gridded = jnp.fft.ifft(gridded, axis=1)
    if rounded:
        gridded = round_complex(gridded)
    spread = jnp.zeros((NX, NY, KZ, KT), mode_values.dtype).at[kept_index(KX, NX)].set(gridded)
    spread = jnp.fft.ifft(spread, axis=0)
    if rounded:
        spread = round_complex(spread)
    plane = jnp.zeros((NX, NY, NZ, NT), mode_values.dtype).at[:, :, kept_index(KZ, NZ), :KT].set(spread)
    return jnp.fft.ifft2(plane, axes=(2, 3)).real.reshape(NX, NY, NZ * NT)

def mix_modes(spectrum, weights):
    shaped = weights.astype(jnp.float32).reshape(2, C, C, KX, KZ, KT, KY)
    conj_weights = lax.complex(shaped[0], -shaped[1])
    return jnp.einsum('oxyzt,oixzty->ixyzt', spectrum, conj_weights)

def sample_grad(cot_sample, pre_sample, spectral_weights, skip_weights, lift_weights):
    incoming = cot_sample.astype(jnp.float32)
    for level_index in range(LAYERS - 1, -1, -1):
        grad_pre = (incoming * gelu_slope(pre_sample[level_index].astype(jnp.float32))).astype(jnp.bfloat16)
        spectrum = lax.map(forward_field, grad_pre)
        mode_values = mix_modes(spectrum, spectral_weights[level_index])
        if level_index > 0:
            mode_values = round_complex(mode_values)
            spectral = lax.map(lambda entry: inverse_field(entry, True), mode_values)
        else:
            spectral = lax.map(lambda entry: inverse_field(entry, False), mode_values)
        skip_term = jnp.einsum('oxyz,oi->ixyz', grad_pre.astype(jnp.float32), skip_weights[level_index].astype(jnp.float32), precision=lax.Precision.HIGHEST)
        incoming = skip_term + spectral
    return jnp.einsum('cxyz,c->xyz', incoming, lift_weights, precision=lax.Precision.HIGHEST)

def reference(cotangent, pre_activations, spectral_weights, skip_weights, lift_weights):

    def one_sample(sample_index):
        cot_sample = lax.dynamic_index_in_dim(cotangent, sample_index, 0, keepdims=False)
        pre_sample = lax.dynamic_index_in_dim(pre_activations, sample_index, 1, keepdims=False)
        return sample_grad(cot_sample, pre_sample, spectral_weights, skip_weights, lift_weights)
    return lax.map(one_sample, jnp.arange(B, dtype=jnp.int32))
```

```python
import functools
import math

import jax
import jax.numpy as jnp
import numpy as np
from jax import lax
from jax.experimental import pallas as pl
from jax.experimental.pallas import tpu as pltpu
from jax.sharding import PartitionSpec as P

NX = 64
NY = 64
NZ = 64
NT = 32
KX = 24
KY = 24
KZ = 24
KT = 12


def gelu_slope(values):
    normal_cdf = 0.5 * (1.0 + lax.erf(values / math.sqrt(2.0)))
    density = jnp.exp(-0.5 * values * values) / math.sqrt(2.0 * math.pi)
    return normal_cdf + values * density


def signed_freq(total_count):
    index_list = np.arange(total_count)
    return np.where(index_list < total_count // 2, index_list, index_list - total_count)


def line_tables(total_count, length):
    turns = signed_freq(total_count)[:, None] * np.arange(length)[None, :] % length
    angles = 2.0 * math.pi / length * turns
    cosine = np.cos(angles)
    sine_part = np.sin(angles)
    forward = np.stack(
        [np.stack([cosine.T, -sine_part.T], 1), np.stack([sine_part.T, cosine.T], 1)], 0
    )
    inverse = (
        np.stack([np.stack([cosine, sine_part], 1), np.stack([-sine_part, cosine], 1)], 0)
        / length
    )
    return (forward, inverse)


def plane_tables():
    joint_index = np.arange(KZ * KT)
    depth_freq = signed_freq(KZ)[joint_index // KT]
    time_freq = joint_index % KT
    cell_index = np.arange(NZ * NT)
    turns = (
        depth_freq[:, None] * (cell_index // NT)[None, :] * NT
        + time_freq[:, None] * (cell_index % NT)[None, :] * NZ
    ) % (NZ * NT)
    angles = 2.0 * math.pi / (NZ * NT) * turns
    forward = np.stack([np.cos(angles).T, -np.sin(angles).T], 1)
    inverse = np.stack([np.cos(angles), -np.sin(angles)], 0) / (NZ * NT)
    return (forward, inverse)


def rounded_product(pattern, values, table):
    return jnp.einsum(
        pattern, values, jnp.asarray(table, jnp.bfloat16), preferred_element_type=jnp.float32
    )


def exact_product(pattern, values, table):
    return jnp.einsum(
        pattern, values, jnp.asarray(table, jnp.float32), precision=lax.Precision.HIGHEST
    )


def to_bf16(values):
    return values.astype(jnp.bfloat16)


def keep_float(values):
    return values


def exchange(values, axis):
    return lax.all_to_all(values, axis, split_axis=0, concat_axis=0, tiled=True)


def forward_modes(grad_pre, weights, tables):
    plane, first, second = tables
    rows = lax.axis_size("aa")
    columns = lax.axis_size("ba")
    plane = plane.reshape(NZ * NT, 2, rows, -1)
    spectrum = to_bf16(rounded_product("bcxyz,zpnm->nbcpxmy", grad_pre, plane))
    blocks = exchange(spectrum, "aa")
    first = first.reshape(2, rows, NX // rows, 2, columns, KX // columns)
    spectrum = to_bf16(rounded_product("nbcpxmy,pnxqgk->gbcqkmy", blocks, first))
    blocks = exchange(spectrum, "ba")
    second = second.reshape(2, columns, NY // columns, 2, KY)
    result = to_bf16(rounded_product("gbcpkmy,pgyqj->bcqkmj", blocks, second))
    shape = result.shape
    spectrum = result.reshape(shape[:4] + (shape[4] * KY,))
    real_part = spectrum[:, :, 0]
    imag_part = spectrum[:, :, 1]

    def mixing(values, matrix):
        return jnp.einsum("bokr,oikr->bikr", values, matrix, preferred_element_type=jnp.float32)

    result_real = mixing(real_part, weights[0]) + mixing(imag_part, weights[1])
    result_imag = mixing(imag_part, weights[0]) - mixing(real_part, weights[1])
    return jnp.stack([result_real, result_imag], 2)


def back_path(mode_values, tables, multiply, finish):
    first, second, plane = tables
    rows = lax.axis_size("aa")
    columns = lax.axis_size("ba")
    extent = mode_values.shape
    gridded = mode_values.reshape(extent[:4] + (extent[4] // KY, KY))
    second = second.reshape(2, KY, 2, columns, NY // columns)
    blocks = exchange(finish(multiply("bcpkmj,pjqgu->gbcqkmu", gridded, second)), "ba")
    first = first.reshape(2, columns, KX // columns, 2, rows, NX // rows)
    back = to_bf16(multiply("gbcpkmu,pgkqnx->nbcqxmu", blocks, first))
    blocks = exchange(back, "aa")
    plane = plane.reshape(2, rows, -1, NZ * NT)
    return rounded_product("nbcpxmu,pnmz->bcxuz", blocks, plane)


def per_device_plain(cotangent, pre_activations, spectral_weights, skip_weights, lift_weights):
    plane_forward, plane_inverse = plane_tables()
    first_forward, first_inverse = line_tables(KX, NX)
    second_forward, second_inverse = line_tables(KY, NY)
    forward_tables = (plane_forward, first_forward, second_forward)
    back_tables = (first_inverse, second_inverse, plane_inverse)
    incoming = cotangent.astype(jnp.float32)
    layers = pre_activations.shape[0]
    perm_grad = None
    for layer_index in range(layers - 1, -1, -1):
        slope = gelu_slope(pre_activations[layer_index].astype(jnp.float32))
        grad_pre = (incoming * slope).astype(jnp.bfloat16)
        mode_values = forward_modes(grad_pre, spectral_weights[layer_index], forward_tables)
        if layer_index > 0:
            skip_term = jnp.einsum(
                "boxyz,oi->bixyz",
                grad_pre,
                skip_weights[layer_index],
                preferred_element_type=jnp.float32,
            )
            spectral = back_path(
                mode_values.astype(jnp.bfloat16), back_tables, rounded_product, to_bf16
            )
            incoming = skip_term + spectral
        else:
            folded = jnp.sum(mode_values * lift_weights[None, :, None, None, None], 1)[:, None]
            spectral = back_path(folded, back_tables, exact_product, keep_float)
            combined = jnp.sum(skip_weights[0].astype(jnp.float32) * lift_weights[None, :], 1)
            projected = jnp.sum(
                grad_pre.astype(jnp.float32) * combined[None, :, None, None, None], 1
            )
            perm_grad = projected + spectral[:, 0]
    return perm_grad


F32 = jnp.float32
BF16 = jnp.bfloat16
MESH = pl.DeviceIdType.MESH


class Plan:
    def __init__(self, mesh, channels):
        self.rows = mesh.shape["aa"]
        self.columns = mesh.shape["ba"]
        self.xb = NX // self.rows
        self.yb = NY // self.columns
        self.mb = KZ * KT // self.rows
        self.kb = KX // self.columns
        self.cells = NZ * NT
        self.spots = self.xb * self.yb
        self.channels = channels
        self.group = 4
        self.groups = channels // self.group
        self.tall = self.group * self.mb
        self.half = 128
        self.kpad = self.half // self.yb
        self.modes = 2 * self.kb * KY

    def fits(self):
        return (
            self.spots == self.half
            and self.half % self.yb == 0
            and self.yb % 16 == 0
            and self.kb <= self.kpad
            and self.channels % self.group == 0
            and self.tall % 16 == 0
            and self.xb % 2 == 0
        )


def real_form(matrix):
    top = np.stack([matrix.real, matrix.imag], 1)
    low = np.stack([-matrix.imag, matrix.real], 1)
    return np.stack([top, low], 0)


def line_phase(count, length):
    turns = signed_freq(count)[:, None] * np.arange(length)[None, :] % length
    return np.exp(2j * math.pi * turns / length)


def dense_tables(plan):
    rows, columns = plan.rows, plan.columns
    eye_y = np.eye(plan.yb)
    eye_k = np.eye(plan.kpad)[: plan.kb]
    along_x = line_phase(KX, NX)
    along_y = line_phase(KY, NY)
    plane_forward, plane_inverse = plane_tables()
    tables = {}
    tables["plane_in"] = plane_forward.transpose(1, 2, 0).reshape(2 * KZ * KT, plan.cells)
    part = real_form(along_x.conj().T).reshape(2, rows, plan.xb, 2, columns, plan.kb)
    wide = np.einsum("psxqgk,yw,kl->spxygqlw", part, eye_y, eye_k)
    tables["x_in"] = wide.reshape(rows * 2 * plan.spots, columns * 2 * plan.half)
    part = real_form(along_y.conj().T).reshape(2, columns, plan.yb, 2, KY)
    wide = np.einsum("pbyqj,kl->bplyqkj", part, eye_k)
    tables["y_in"] = wide.reshape(columns * 2 * plan.half, plan.modes)
    part = (real_form(along_y) / NY).reshape(2, KY, 2, columns, plan.yb)
    wide = np.einsum("pjqhy,kl->pkjhqly", part, eye_k)
    tables["y_out"] = wide.reshape(plan.modes, columns * 2 * plan.half)
    part = (real_form(along_x) / NX).reshape(2, columns, plan.kb, 2, rows, plan.xb)
    wide = np.einsum("pbkqnx,yw,kl->bplynqxw", part, eye_y, eye_k)
    tables["x_out"] = wide.reshape(columns * 2 * plan.half, rows * 2 * plan.spots)
    back = plane_inverse.reshape(2, rows, plan.mb, plan.cells).transpose(1, 0, 2, 3)
    tables["plane_out"] = back.reshape(2 * KZ * KT, plan.cells)
    return {name: jnp.asarray(table.astype(jnp.bfloat16)) for name, table in tables.items()}


def product(left, right, contract=((1,), (0,))):
    return lax.dot_general(left, right, (contract, ((), ())), preferred_element_type=F32)


def greet(plan):
    barrier = pltpu.get_barrier_semaphore()
    for axis, size in (("aa", plan.rows), ("ba", plan.columns)):
        for hop in range(1, size):
            peer = lax.rem(lax.axis_index(axis) + hop, size)
            pl.semaphore_signal(barrier, inc=1, device_id={axis: peer}, device_id_type=MESH)
    pl.semaphore_wait(barrier, plan.rows + plan.columns - 2)


class Exchange:
    def __init__(self, axis, size, out, into, sent, came):
        self.axis, self.size = axis, size
        self.out, self.into, self.sent, self.came = out, into, sent, came

    def copy(self, group, hop):
        me = lax.axis_index(self.axis)
        peer = lax.rem(me + hop, self.size)
        return pltpu.make_async_remote_copy(
            src_ref=self.out.at[group, peer],
            dst_ref=self.into.at[group, me],
            send_sem=self.sent.at[group, hop],
            recv_sem=self.came.at[group, hop],
            device_id={self.axis: peer},
            device_id_type=MESH,
        )

    def start(self, group):
        for hop in range(1, self.size):
            self.copy(group, hop).start()
        me = lax.axis_index(self.axis)
        self.into[group, me] = self.out[group, me]

    def arrive(self, group):
        for hop in range(1, self.size):
            self.copy(group, hop).wait_recv()

    def finish(self, groups):
        def drain(group, carry):
            for hop in range(1, self.size):
                self.copy(group, hop).wait_send()
            return carry

        lax.fori_loop(0, groups, drain, 0)


def exchange_scratch(plan, groups, tall):
    rows, columns = plan.rows, plan.columns
    return [
        pltpu.VMEM((groups, rows, tall, 2 * plan.spots), BF16),
        pltpu.VMEM((groups, rows, tall, 2 * plan.spots), BF16),
        pltpu.SemaphoreType.DMA((groups, rows)),
        pltpu.SemaphoreType.DMA((groups, rows)),
        pltpu.VMEM((groups, columns, tall, 2 * plan.half), BF16),
        pltpu.VMEM((groups, columns, tall, 2 * plan.half), BF16),
        pltpu.SemaphoreType.DMA((groups, columns)),
        pltpu.SemaphoreType.DMA((groups, columns)),
    ]


def exchanges(plan, scratch):
    return (
        Exchange("aa", plan.rows, *scratch[:4]),
        Exchange("ba", plan.columns, *scratch[4:8]),
    )


def plane_in(plan, group, values, table, wide, over_a):
    rows, mb, spots = plan.rows, plan.mb, plan.spots
    wide[...] = product(table[...], values, ((1,), (1,)))
    for owner in range(rows):
        halves = []
        for part in range(2):
            first = (part * rows + owner) * mb
            halves.append(
                jnp.concatenate(
                    [
                        wide[first : first + mb, c * spots : (c + 1) * spots]
                        for c in range(plan.group)
                    ],
                    0,
                )
            )
        over_a.out[group, owner] = jnp.concatenate(halves, 1).astype(BF16)
    over_a.start(group)


def joined(ref, group, size):
    return jnp.concatenate([ref[group, index] for index in range(size)], 1)


def x_in(plan, group, table, over_a, over_b):
    over_a.arrive(group)
    result = product(joined(over_a.into, group, plan.rows), table[...]).astype(BF16)
    width = 2 * plan.half
    for owner in range(plan.columns):
        over_b.out[group, owner] = result[:, owner * width : (owner + 1) * width]
    over_b.start(group)


def y_in(plan, group, table, over_b, spectrum):
    over_b.arrive(group)
    result = product(joined(over_b.into, group, plan.columns), table[...])
    spectrum[0] = result.astype(BF16)


def y_out(plan, group, values, table, over_b):
    result = product(values, table[...]).astype(BF16)
    width = 2 * plan.half
    for owner in range(plan.columns):
        over_b.out[group, owner] = result[:, owner * width : (owner + 1) * width]
    over_b.start(group)


def x_out(plan, group, table, over_b, over_a):
    over_b.arrive(group)
    values = joined(over_b.into, group, plan.columns)
    width = 2 * plan.spots
    for owner in range(plan.rows):
        cut = table[:, owner * width : (owner + 1) * width]
        over_a.out[group, owner] = product(values, cut).astype(BF16)
    over_a.start(group)


def plane_out(plan, group, count, table, over_a):
    over_a.arrive(group)
    mb, spots = plan.mb, plan.spots
    pieces = []
    for source in range(plan.rows):
        block = over_a.into[group, source].astype(F32)
        for part in range(2):
            pieces.append(
                jnp.concatenate(
                    [
                        block[c * mb : (c + 1) * mb, part * spots : (part + 1) * spots]
                        for c in range(count)
                    ],
                    1,
                )
            )
    values = jnp.concatenate(pieces, 0).astype(BF16)
    return product(values, table[...], ((0,), (0,)))


def forward_kernel(plan, cotangent, pre, t_plane, t_x, t_y, mix, skip, spectrum, field, wide, *scratch):
    step = pl.program_id(0)
    over_a, over_b = exchanges(plan, scratch)
    groups, group = plan.groups, plan.group
    lanes = 512

    @pl.when(step == 0)
    def _():
        greet(plan)

    @pl.when(step < groups)
    def _():
        def line(index, carry):
            c = index // plan.xb
            x = index % plan.xb
            for first in range(0, plan.cells, lanes):
                cut = pl.ds(first, lanes)
                slope = gelu_slope(pre[0, 0, c, x, :, cut].astype(F32))
                value = cotangent[0, c, x, :, cut].astype(F32) * slope
                field[step * group + c, x, :, cut] = value.astype(BF16)
            return carry

        lax.fori_loop(0, group * plan.xb, line, 0)
        values = field[pl.ds(step * group, group)].reshape(group * plan.spots, plan.cells)
        plane_in(plan, step, values, t_plane, wide, over_a)

    @pl.when(step >= groups)
    def _():
        def line(index, carry):
            x = (step - groups) * (plan.xb // 2) + index
            for first in range(0, plan.cells, lanes):
                cut = pl.ds(first, lanes)
                values = field[:, x, :, cut].reshape(plan.channels * plan.yb, lanes)
                result = product(mix[...], values).astype(BF16)
                skip[:, index, :, cut] = result.reshape(plan.channels, plan.yb, lanes)
            return carry

        lax.fori_loop(0, plan.xb // 2, line, 0)

    @pl.when(jnp.logical_and(step >= 1, step <= groups))
    def _():
        x_in(plan, step - 1, t_x, over_a, over_b)

    @pl.when(step >= 2)
    def _():
        y_in(plan, step - 2, t_y, over_b, spectrum)

    @pl.when(step == groups + 1)
    def _():
        over_a.finish(groups)
        over_b.finish(groups)


def middle_kernel(
    plan, modes, skip, pre, weight, t_plane, t_x, t_y, s_y, s_x, s_plane,
    spectrum, projected, values, wide, *scratch,
):
    step = pl.program_id(0)
    back_a, back_b = exchanges(plan, scratch[:8])
    over_a, over_b = exchanges(plan, scratch[8:])
    groups, group = plan.groups, plan.group
    lanes = 512

    @pl.when(step == 0)
    def _():
        greet(plan)

        def send(index, carry):
            y_out(plan, index, modes[index], s_y, back_b)
            return carry

        lax.fori_loop(0, groups, send, 0)
        projected[...] = jnp.zeros_like(projected)

    @pl.when(step < groups)
    def _():
        x_out(plan, step, s_x, back_b, back_a)

    @pl.when(jnp.logical_and(step >= 1, step <= groups))
    def _():
        at = step - 1
        values[...] = plane_out(plan, at, group, s_plane, back_a)

        def line(index, carry):
            c = index // plan.xb
            x = index % plan.xb
            scale = weight[at * group + c]
            row = pl.multiple_of(index * plan.yb, plan.yb)
            spot = pl.multiple_of(x * plan.yb, plan.yb)
            for first in range(0, plan.cells, lanes):
                cut = pl.ds(first, lanes)
                slope = gelu_slope(pre[0, 0, c, x, :, cut].astype(F32))
                incoming = values[pl.ds(row, plan.yb), cut] + skip[c, x, :, cut].astype(F32)
                value = (incoming * slope).astype(BF16)
                fields_ref = wide[1]
                fields_ref[pl.ds(row, plan.yb), cut] = value
                projected[pl.ds(spot, plan.yb), cut] += value.astype(F32) * scale
            return carry

        lax.fori_loop(0, group * plan.xb, line, 0)
        plane_in(plan, at, wide[1][...], t_plane, wide[0], over_a)

    @pl.when(jnp.logical_and(step >= 2, step <= groups + 1))
    def _():
        x_in(plan, step - 2, t_x, over_a, over_b)

    @pl.when(step >= 3)
    def _():
        y_in(plan, step - 3, t_y, over_b, spectrum)

    @pl.when(step == groups + 2)
    def _():
        for each in (back_a, back_b, over_a, over_b):
            each.finish(groups)


def middle_entry(plan, *refs):
    middle_kernel(plan, *refs[:13], (refs[13], refs[14]), *refs[15:])


def tail_kernel(plan, modes, projected, s_y, s_x, s_plane, result, *scratch):
    over_a, over_b = exchanges(plan, scratch)
    greet(plan)
    y_out(plan, 0, modes[0], s_y, over_b)
    x_out(plan, 0, s_x, over_b, over_a)
    result[...] = projected[...] + plane_out(plan, 0, 1, s_plane, over_a)
    over_a.finish(1)
    over_b.finish(1)


def whole():
    return pl.BlockSpec(memory_space=pltpu.VMEM, pipeline_mode=pl.Buffered(1))


VMEM_LIMIT = 62 * 1024 * 1024


def forward_call(plan, layer, cotangent, pre_activations, tables, mix):
    groups, group = plan.groups, plan.group
    field = (plan.xb, plan.yb, plan.cells)

    def at_group(step):
        return jnp.minimum(step, groups - 1)

    return pl.pallas_call(
        functools.partial(forward_kernel, plan),
        grid=(groups + 2,),
        in_specs=[
            pl.BlockSpec((1, group) + field, lambda s: (0, at_group(s), 0, 0, 0)),
            pl.BlockSpec((1, 1, group) + field, lambda s: (layer, 0, at_group(s), 0, 0, 0)),
            whole(),
            whole(),
            whole(),
            whole(),
        ],
        out_specs=[
            pl.BlockSpec(
                (plan.channels, plan.xb // 2, plan.yb, plan.cells),
                lambda s: (0, jnp.clip(s - groups, 0, 1), 0, 0),
            ),
            pl.BlockSpec(
                (1, plan.tall, plan.modes), lambda s: (jnp.clip(s - 2, 0, groups - 1), 0, 0)
            ),
        ],
        out_shape=[
            jax.ShapeDtypeStruct((plan.channels,) + field, BF16),
            jax.ShapeDtypeStruct((groups, plan.tall, plan.modes), BF16),
        ],
        scratch_shapes=[
            pltpu.VMEM((plan.channels,) + field, BF16),
            pltpu.VMEM((2 * KZ * KT, group * plan.spots), F32),
        ]
        + exchange_scratch(plan, groups, plan.tall),
        compiler_params=pltpu.CompilerParams(
            collective_id=1, has_side_effects=True, vmem_limit_bytes=VMEM_LIMIT
        ),
        name="forward",
    )(cotangent, pre_activations, tables["plane_in"], tables["x_in"], tables["y_in"], mix)


def middle_call(plan, layer, modes, skip, pre_activations, weight, tables):
    groups, group = plan.groups, plan.group
    field = (plan.xb, plan.yb, plan.cells)

    def at_group(step):
        return jnp.clip(step - 1, 0, groups - 1)

    names = ("plane_in", "x_in", "y_in", "y_out", "x_out", "plane_out")
    return pl.pallas_call(
        functools.partial(middle_entry, plan),
        grid=(groups + 3,),
        in_specs=[
            whole(),
            pl.BlockSpec((group,) + field, lambda s: (at_group(s), 0, 0, 0)),
            pl.BlockSpec((1, 1, group) + field, lambda s: (layer, 0, at_group(s), 0, 0, 0)),
            pl.BlockSpec(memory_space=pltpu.SMEM),
        ]
        + [whole()] * len(names),
        out_specs=[
            pl.BlockSpec(
                (1, plan.tall, plan.modes), lambda s: (jnp.clip(s - 3, 0, groups - 1), 0, 0)
            ),
            pl.BlockSpec((plan.spots, plan.cells), lambda s: (0, 0)),
        ],
        out_shape=[
            jax.ShapeDtypeStruct((groups, plan.tall, plan.modes), BF16),
            jax.ShapeDtypeStruct((plan.spots, plan.cells), F32),
        ],
        scratch_shapes=[
            pltpu.VMEM((group * plan.spots, plan.cells), F32),
            pltpu.VMEM((2 * KZ * KT, group * plan.spots), F32),
            pltpu.VMEM((group * plan.spots, plan.cells), BF16),
        ]
        + exchange_scratch(plan, groups, plan.tall)
        + exchange_scratch(plan, groups, plan.tall),
        compiler_params=pltpu.CompilerParams(
            collective_id=2, has_side_effects=True, vmem_limit_bytes=VMEM_LIMIT
        ),
        name="middle",
    )(modes, skip, pre_activations, weight, *[tables[name] for name in names])


def tail_call(plan, modes, projected, tables):
    tall = modes.shape[1]
    names = ("y_out", "x_out", "plane_out")
    return pl.pallas_call(
        functools.partial(tail_kernel, plan),
        in_specs=[pl.BlockSpec(memory_space=pltpu.VMEM)] * 5,
        out_specs=pl.BlockSpec(memory_space=pltpu.VMEM),
        out_shape=jax.ShapeDtypeStruct((plan.spots, plan.cells), F32),
        scratch_shapes=exchange_scratch(plan, 1, tall),
        compiler_params=pltpu.CompilerParams(
            collective_id=3, has_side_effects=True, vmem_limit_bytes=VMEM_LIMIT
        ),
        name="tail",
    )(modes, projected, *[tables[name] for name in names])


def by_frequency(plan, spectrum):
    gridded = spectrum.reshape(plan.channels, plan.mb, 2, plan.kb, KY)
    turned = gridded.transpose(2, 0, 3, 1, 4)
    return turned.reshape(2, plan.channels, plan.kb, plan.mb * KY).astype(F32)


def per_device(plan, cotangent, pre_activations, spectral_weights, skip_weights, lift_weights):
    tables = dense_tables(plan)
    mix = jnp.kron(skip_weights[1].T, jnp.eye(plan.yb, dtype=BF16))
    skip, spectrum = forward_call(plan, 1, cotangent, pre_activations, tables, mix)

    def mixing(values, matrix):
        return jnp.sum(values[:, None] * matrix.astype(F32), 0)

    spectrum = by_frequency(plan, spectrum)
    upper = spectral_weights[1]
    real = mixing(spectrum[0], upper[0]) + mixing(spectrum[1], upper[1])
    imag = mixing(spectrum[1], upper[0]) - mixing(spectrum[0], upper[1])
    modes = jnp.stack([real, imag]).astype(BF16)
    modes = modes.reshape(2, plan.channels, plan.kb, plan.mb, KY).transpose(1, 3, 0, 2, 4)
    modes = modes.reshape(plan.groups, plan.tall, plan.modes)
    weight = jnp.sum(skip_weights[0].astype(F32) * lift_weights[None, :], 1)
    spectrum, projected = middle_call(plan, 0, modes, skip, pre_activations, weight, tables)

    spectrum = by_frequency(plan, spectrum)
    lifted = lift_weights[None, None, :, None, None]
    lower = jnp.sum(spectral_weights[0].astype(F32) * lifted, 2)
    real = jnp.sum(spectrum[0] * lower[0] + spectrum[1] * lower[1], 0)
    imag = jnp.sum(spectrum[1] * lower[0] - spectrum[0] * lower[1], 0)
    modes = jnp.stack([real, imag]).reshape(2, plan.kb, plan.mb, KY).transpose(2, 0, 1, 3)
    modes = modes.reshape(1, plan.mb, plan.modes).astype(BF16)
    modes = jnp.pad(modes, ((0, 0), (0, -plan.mb % 16), (0, 0)))
    result = tail_call(plan, modes, projected, tables)
    return result.reshape(1, plan.xb, plan.yb, plan.cells)


def solution(mesh):
    def step(cotangent, pre_activations, spectral_weights, skip_weights, lift_weights):
        plan = Plan(mesh, cotangent.shape[1])
        layers, samples = pre_activations.shape[:2]
        if layers == 2 and samples == 1 and plan.fits():
            body = functools.partial(per_device, plan)
        else:
            body = per_device_plain
        return body(cotangent, pre_activations, spectral_weights, skip_weights, lift_weights)

    return jax.shard_map(
        step,
        mesh=mesh,
        in_specs=(
            P(None, None, "aa", "ba", None),
            P(None, None, None, "aa", "ba", None),
            P(None, None, None, None, "ba", "aa"),
            P(),
            P(),
        ),
        out_specs=P(None, "aa", "ba", None),
        check_vma=False,
    )
```

```python
import functools
import math

import jax
import jax.numpy as jnp
import numpy as np
from jax import lax
from jax.experimental import pallas as pl
from jax.experimental.pallas import tpu as pltpu
from jax.sharding import PartitionSpec as P

NX = 64
NY = 64
NZ = 64
NT = 32
KX = 24
KY = 24
KZ = 24
KT = 12


def gelu_slope(values):
    normal_cdf = 0.5 * (1.0 + lax.erf(values / math.sqrt(2.0)))
    density = jnp.exp(-0.5 * values * values) / math.sqrt(2.0 * math.pi)
    return normal_cdf + values * density


def signed_freq(total_count):
    index_list = np.arange(total_count)
    return np.where(index_list < total_count // 2, index_list, index_list - total_count)


def line_tables(total_count, length):
    turns = signed_freq(total_count)[:, None] * np.arange(length)[None, :] % length
    angles = 2.0 * math.pi / length * turns
    cosine = np.cos(angles)
    sine_part = np.sin(angles)
    forward = np.stack(
        [np.stack([cosine.T, -sine_part.T], 1), np.stack([sine_part.T, cosine.T], 1)], 0
    )
    inverse = (
        np.stack([np.stack([cosine, sine_part], 1), np.stack([-sine_part, cosine], 1)], 0)
        / length
    )
    return (forward, inverse)


def plane_tables():
    joint_index = np.arange(KZ * KT)
    depth_freq = signed_freq(KZ)[joint_index // KT]
    time_freq = joint_index % KT
    cell_index = np.arange(NZ * NT)
    turns = (
        depth_freq[:, None] * (cell_index // NT)[None, :] * NT
        + time_freq[:, None] * (cell_index % NT)[None, :] * NZ
    ) % (NZ * NT)
    angles = 2.0 * math.pi / (NZ * NT) * turns
    forward = np.stack([np.cos(angles).T, -np.sin(angles).T], 1)
    inverse = np.stack([np.cos(angles), -np.sin(angles)], 0) / (NZ * NT)
    return (forward, inverse)


def rounded_product(pattern, values, table):
    return jnp.einsum(
        pattern, values, jnp.asarray(table, jnp.bfloat16), preferred_element_type=jnp.float32
    )


def exact_product(pattern, values, table):
    return jnp.einsum(
        pattern, values, jnp.asarray(table, jnp.float32), precision=lax.Precision.HIGHEST
    )


def to_bf16(values):
    return values.astype(jnp.bfloat16)


def keep_float(values):
    return values


def exchange(values, axis):
    return lax.all_to_all(values, axis, split_axis=0, concat_axis=0, tiled=True)


def forward_modes(grad_pre, weights, tables):
    plane, first, second = tables
    rows = lax.axis_size("aa")
    columns = lax.axis_size("ba")
    plane = plane.reshape(NZ * NT, 2, rows, -1)
    spectrum = to_bf16(rounded_product("bcxyz,zpnm->nbcpxmy", grad_pre, plane))
    blocks = exchange(spectrum, "aa")
    first = first.reshape(2, rows, NX // rows, 2, columns, KX // columns)
    spectrum = to_bf16(rounded_product("nbcpxmy,pnxqgk->gbcqkmy", blocks, first))
    blocks = exchange(spectrum, "ba")
    second = second.reshape(2, columns, NY // columns, 2, KY)
    result = to_bf16(rounded_product("gbcpkmy,pgyqj->bcqkmj", blocks, second))
    shape = result.shape
    spectrum = result.reshape(shape[:4] + (shape[4] * KY,))
    real_part = spectrum[:, :, 0]
    imag_part = spectrum[:, :, 1]

    def mixing(values, matrix):
        return jnp.einsum("bokr,oikr->bikr", values, matrix, preferred_element_type=jnp.float32)

    result_real = mixing(real_part, weights[0]) + mixing(imag_part, weights[1])
    result_imag = mixing(imag_part, weights[0]) - mixing(real_part, weights[1])
    return jnp.stack([result_real, result_imag], 2)


def back_path(mode_values, tables, multiply, finish):
    first, second, plane = tables
    rows = lax.axis_size("aa")
    columns = lax.axis_size("ba")
    extent = mode_values.shape
    gridded = mode_values.reshape(extent[:4] + (extent[4] // KY, KY))
    second = second.reshape(2, KY, 2, columns, NY // columns)
    blocks = exchange(finish(multiply("bcpkmj,pjqgu->gbcqkmu", gridded, second)), "ba")
    first = first.reshape(2, columns, KX // columns, 2, rows, NX // rows)
    back = to_bf16(multiply("gbcpkmu,pgkqnx->nbcqxmu", blocks, first))
    blocks = exchange(back, "aa")
    plane = plane.reshape(2, rows, -1, NZ * NT)
    return rounded_product("nbcpxmu,pnmz->bcxuz", blocks, plane)


def per_device_plain(cotangent, pre_activations, spectral_weights, skip_weights, lift_weights):
    plane_forward, plane_inverse = plane_tables()
    first_forward, first_inverse = line_tables(KX, NX)
    second_forward, second_inverse = line_tables(KY, NY)
    forward_tables = (plane_forward, first_forward, second_forward)
    back_tables = (first_inverse, second_inverse, plane_inverse)
    incoming = cotangent.astype(jnp.float32)
    layers = pre_activations.shape[0]
    perm_grad = None
    for layer_index in range(layers - 1, -1, -1):
        slope = gelu_slope(pre_activations[layer_index].astype(jnp.float32))
        grad_pre = (incoming * slope).astype(jnp.bfloat16)
        mode_values = forward_modes(grad_pre, spectral_weights[layer_index], forward_tables)
        if layer_index > 0:
            skip_term = jnp.einsum(
                "boxyz,oi->bixyz",
                grad_pre,
                skip_weights[layer_index],
                preferred_element_type=jnp.float32,
            )
            spectral = back_path(
                mode_values.astype(jnp.bfloat16), back_tables, rounded_product, to_bf16
            )
            incoming = skip_term + spectral
        else:
            folded = jnp.sum(mode_values * lift_weights[None, :, None, None, None], 1)[:, None]
            spectral = back_path(folded, back_tables, exact_product, keep_float)
            combined = jnp.sum(skip_weights[0].astype(jnp.float32) * lift_weights[None, :], 1)
            projected = jnp.sum(
                grad_pre.astype(jnp.float32) * combined[None, :, None, None, None], 1
            )
            perm_grad = projected + spectral[:, 0]
    return perm_grad


F32 = jnp.float32
BF16 = jnp.bfloat16
MESH = pl.DeviceIdType.MESH


class Plan:
    def __init__(self, mesh, channels):
        self.rows = mesh.shape["aa"]
        self.columns = mesh.shape["ba"]
        self.xb = NX // self.rows
        self.yb = NY // self.columns
        self.mb = KZ * KT // self.rows
        self.kb = KX // self.columns
        self.cells = NZ * NT
        self.spots = self.xb * self.yb
        self.channels = channels
        self.group = 4
        self.groups = channels // self.group
        self.tall = self.group * self.mb
        self.half = 128
        self.kpad = self.half // self.yb
        self.modes = self.kb * KY
        self.room = -(-self.modes // 128) * 128
        self.lines = self.mb * KY

    def fits(self):
        return (
            self.spots == self.half
            and self.half % self.yb == 0
            and self.yb % 16 == 0
            and self.kb <= self.kpad
            and self.channels % self.group == 0
            and self.tall % 16 == 0
            and self.xb % 2 == 0
        )


def real_form(matrix):
    top = np.stack([matrix.real, matrix.imag], 1)
    low = np.stack([-matrix.imag, matrix.real], 1)
    return np.stack([top, low], 0)


def line_phase(count, length):
    turns = signed_freq(count)[:, None] * np.arange(length)[None, :] % length
    return np.exp(2j * math.pi * turns / length)


def dense_tables(plan):
    rows, columns = plan.rows, plan.columns
    eye_y = np.eye(plan.yb)
    eye_k = np.eye(plan.kpad)[: plan.kb]
    along_x = line_phase(KX, NX)
    along_y = line_phase(KY, NY)
    plane_forward, plane_inverse = plane_tables()
    tables = {}
    tables["plane_in"] = plane_forward.transpose(1, 2, 0).reshape(2 * KZ * KT, plan.cells)
    part = real_form(along_x.conj().T).reshape(2, rows, plan.xb, 2, columns, plan.kb)
    wide = np.einsum("psxqgk,yw,kl->spxygqlw", part, eye_y, eye_k)
    tables["x_in"] = wide.reshape(rows * 2 * plan.spots, columns * 2 * plan.half)
    part = real_form(along_y.conj().T).reshape(2, columns, plan.yb, 2, KY)
    wide = np.einsum("pbyqj,kl->bplyqkj", part, eye_k)
    wide = wide.reshape(columns * 2 * plan.half, 2, plan.modes)
    wide = np.pad(wide, ((0, 0), (0, 0), (0, plan.room - plan.modes)))
    tables["y_in"] = wide.reshape(columns * 2 * plan.half, 2 * plan.room)
    part = (real_form(along_y) / NY).reshape(2, KY, 2, columns, plan.yb)
    wide = np.einsum("pjqhy,kl->pkjhqly", part, eye_k)
    tables["y_out"] = wide.reshape(2, plan.modes, columns * 2 * plan.half)
    part = (real_form(along_x) / NX).reshape(2, columns, plan.kb, 2, rows, plan.xb)
    wide = np.einsum("pbkqnx,yw,kl->bplynqxw", part, eye_y, eye_k)
    tables["x_out"] = wide.reshape(columns * 2 * plan.half, rows * 2 * plan.spots)
    back = plane_inverse.reshape(2, rows, plan.mb, plan.cells).transpose(1, 0, 2, 3)
    tables["plane_out"] = back.reshape(2 * KZ * KT, plan.cells)
    return {name: jnp.asarray(table.astype(jnp.bfloat16)) for name, table in tables.items()}


def product(left, right, contract=((1,), (0,))):
    return lax.dot_general(left, right, (contract, ((), ())), preferred_element_type=F32)


def greet(plan):
    barrier = pltpu.get_barrier_semaphore()
    for axis, size in (("aa", plan.rows), ("ba", plan.columns)):
        for hop in range(1, size):
            peer = lax.rem(lax.axis_index(axis) + hop, size)
            pl.semaphore_signal(barrier, inc=1, device_id={axis: peer}, device_id_type=MESH)
    pl.semaphore_wait(barrier, plan.rows + plan.columns - 2)


class Exchange:
    def __init__(self, axis, size, out, into, sent, came):
        self.axis, self.size = axis, size
        self.out, self.into, self.sent, self.came = out, into, sent, came

    def copy(self, group, hop):
        me = lax.axis_index(self.axis)
        peer = lax.rem(me + hop, self.size)
        return pltpu.make_async_remote_copy(
            src_ref=self.out.at[group, peer],
            dst_ref=self.into.at[group, me],
            send_sem=self.sent.at[group, hop],
            recv_sem=self.came.at[group, hop],
            device_id={self.axis: peer},
            device_id_type=MESH,
        )

    def start(self, group):
        for hop in range(1, self.size):
            self.copy(group, hop).start()
        me = lax.axis_index(self.axis)
        self.into[group, me] = self.out[group, me]

    def arrive(self, group):
        for hop in range(1, self.size):
            self.copy(group, hop).wait_recv()

    def finish(self, groups):
        def drain(group, carry):
            for hop in range(1, self.size):
                self.copy(group, hop).wait_send()
            return carry

        lax.fori_loop(0, groups, drain, 0)


def exchange_scratch(plan, groups, tall):
    rows, columns = plan.rows, plan.columns
    return [
        pltpu.VMEM((groups, rows, tall, 2 * plan.spots), BF16),
        pltpu.VMEM((groups, rows, tall, 2 * plan.spots), BF16),
        pltpu.SemaphoreType.DMA((groups, rows)),
        pltpu.SemaphoreType.DMA((groups, rows)),
        pltpu.VMEM((groups, columns, tall, 2 * plan.half), BF16),
        pltpu.VMEM((groups, columns, tall, 2 * plan.half), BF16),
        pltpu.SemaphoreType.DMA((groups, columns)),
        pltpu.SemaphoreType.DMA((groups, columns)),
    ]


def exchanges(plan, scratch):
    return (
        Exchange("aa", plan.rows, *scratch[:4]),
        Exchange("ba", plan.columns, *scratch[4:8]),
    )


def plane_in(plan, group, values, table, wide, over_a):
    rows, mb, spots = plan.rows, plan.mb, plan.spots
    wide[...] = product(table[...], values, ((1,), (1,)))
    for owner in range(rows):
        halves = []
        for part in range(2):
            first = (part * rows + owner) * mb
            halves.append(
                jnp.concatenate(
                    [
                        wide[first : first + mb, c * spots : (c + 1) * spots]
                        for c in range(plan.group)
                    ],
                    0,
                )
            )
        over_a.out[group, owner] = jnp.concatenate(halves, 1).astype(BF16)
    over_a.start(group)


def joined(ref, group, size):
    return jnp.concatenate([ref[group, index] for index in range(size)], 1)


def x_in(plan, group, table, over_a, over_b):
    over_a.arrive(group)
    result = product(joined(over_a.into, group, plan.rows), table[...]).astype(BF16)
    width = 2 * plan.half
    for owner in range(plan.columns):
        over_b.out[group, owner] = result[:, owner * width : (owner + 1) * width]
    over_b.start(group)


def y_in(plan, group, table, over_b, sheet, real_first, imag_first):
    over_b.arrive(group)
    result = product(joined(over_b.into, group, plan.columns), table[...])
    mb = plan.mb
    for c in range(plan.group):
        for part in range(2):
            lane = part * plan.room
            row = (2 * c + part) * mb
            for half in range(plan.room // 128):
                first = lane + 128 * half
                piece = result[c * mb : (c + 1) * mb, first : first + 128]
                sheet[half, row : row + mb] = piece
    count = 2 * plan.group
    lines = []
    for m in range(mb):
        row = pl.ds(m, count, stride=mb)
        lines.append(jnp.concatenate([sheet[h, row, :] for h in range(plan.room // 128)], 1))
    for k in range(plan.kb):
        turned = jnp.concatenate([line[:, k * KY : (k + 1) * KY] for line in lines], 1)
        for c in range(plan.group):
            real = turned[2 * c : 2 * c + 1]
            imag = turned[2 * c + 1 : 2 * c + 2]
            real_first[c, k] = jnp.concatenate([real, imag], 0)
            imag_first[c, k] = jnp.concatenate([imag, -real], 0)


def mix_in(plan, weights, real_first, imag_first, real_sum, imag_sum):
    for c in range(plan.group):
        for k in range(plan.kb):
            first = real_first[c, k]
            second = imag_first[c, k]

            def add(i, carry):
                matrix = weights[0, c, i, k].astype(F32)
                real_sum[i, k] += matrix * first
                imag_sum[i, k] += matrix * second
                return carry

            lax.fori_loop(0, plan.channels, add, 0, unroll=10)


def fold_in(plan, group, weights, lift, folded):
    for c in range(plan.group):

        def line(k, carry):
            total = weights[0, c, 0, k].astype(F32) * lift[0]
            for i in range(1, plan.channels):
                total = total + weights[0, c, i, k].astype(F32) * lift[i]
            folded[group * plan.group + c, k] = total
            return carry

        lax.fori_loop(0, plan.kb, line, 0)


def by_row(plan, rows, sheet):
    count = rows[0].shape[0]
    for m in range(plan.mb):
        pieces = [row[:, m * KY : (m + 1) * KY] for row in rows]
        if plan.room > plan.modes:
            pieces.append(jnp.zeros((count, plan.room - plan.modes), F32))
        line = jnp.concatenate(pieces, 1)
        for half in range(plan.room // 128):
            row = pl.ds(m, count, stride=plan.mb)
            sheet[half, row, :] = line[:, half * 128 : (half + 1) * 128]


def sheet_rows(plan, sheet, first, last):
    halves = [sheet[half, first:last] for half in range(plan.room // 128)]
    return jnp.concatenate(halves, 1)[:, : plan.modes].astype(BF16)


def y_out(plan, group, parts, table, over_b):
    result = (product(parts[0], table[0]) + product(parts[1], table[1])).astype(BF16)
    width = 2 * plan.half
    tall = result.shape[0]
    for owner in range(plan.columns):
        cut = result[:, owner * width : (owner + 1) * width]
        if tall < over_b.out.shape[2]:
            over_b.out[group, owner, :tall] = cut
        else:
            over_b.out[group, owner] = cut
    over_b.start(group)


def x_out(plan, group, table, over_b, over_a):
    over_b.arrive(group)
    values = joined(over_b.into, group, plan.columns)
    width = 2 * plan.spots
    for owner in range(plan.rows):
        cut = table[:, owner * width : (owner + 1) * width]
        over_a.out[group, owner] = product(values, cut).astype(BF16)
    over_a.start(group)


def plane_out(plan, group, count, table, over_a):
    over_a.arrive(group)
    mb, spots = plan.mb, plan.spots
    pieces = []
    for source in range(plan.rows):
        block = over_a.into[group, source].astype(F32)
        for part in range(2):
            pieces.append(
                jnp.concatenate(
                    [
                        block[c * mb : (c + 1) * mb, part * spots : (part + 1) * spots]
                        for c in range(count)
                    ],
                    1,
                )
            )
    values = jnp.concatenate(pieces, 0).astype(BF16)
    return product(values, table[...], ((0,), (0,)))


def forward_kernel(
    plan, cotangent, pre, weights, t_plane, t_x, t_y, mix, skip, modes,
    field, wide, sheet, real_first, imag_first, real_sum, imag_sum, *scratch,
):
    step = pl.program_id(0)
    over_a, over_b = exchanges(plan, scratch)
    groups, group = plan.groups, plan.group
    lanes = 512

    @pl.when(step == 0)
    def _():
        greet(plan)
        real_sum[...] = jnp.zeros_like(real_sum)
        imag_sum[...] = jnp.zeros_like(imag_sum)

    @pl.when(step < groups)
    def _():
        def line(index, carry):
            c = index // plan.xb
            x = index % plan.xb
            for first in range(0, plan.cells, lanes):
                cut = pl.ds(first, lanes)
                slope = gelu_slope(pre[0, 0, c, x, :, cut].astype(F32))
                value = cotangent[0, c, x, :, cut].astype(F32) * slope
                field[step * group + c, x, :, cut] = value.astype(BF16)
            return carry

        lax.fori_loop(0, group * plan.xb, line, 0)
        values = field[pl.ds(step * group, group)].reshape(group * plan.spots, plan.cells)
        plane_in(plan, step, values, t_plane, wide, over_a)

    @pl.when(step >= groups)
    def _():
        def line(index, carry):
            x = (step - groups) * (plan.xb // 2) + index
            for first in range(0, plan.cells, lanes):
                cut = pl.ds(first, lanes)
                values = field[:, x, :, cut].reshape(plan.channels * plan.yb, lanes)
                result = product(mix[...], values).astype(BF16)
                skip[:, index, :, cut] = result.reshape(plan.channels, plan.yb, lanes)
            return carry

        lax.fori_loop(0, plan.xb // 2, line, 0)

    @pl.when(jnp.logical_and(step >= 1, step <= groups))
    def _():
        x_in(plan, step - 1, t_x, over_a, over_b)

    @pl.when(step >= 2)
    def _():
        y_in(plan, step - 2, t_y, over_b, sheet, real_first, imag_first)
        mix_in(plan, weights, real_first, imag_first, real_sum, imag_sum)

    @pl.when(step == groups + 1)
    def _():
        def turn(index, carry):
            rows = []
            for k in range(plan.kb):
                row = []
                for total in (real_sum, imag_sum):
                    for c in range(group):
                        both = total[index * group + c, k]
                        row.append(both[:1] + both[1:])
                rows.append(jnp.concatenate(row, 0))
            by_row(plan, rows, sheet)
            modes[index] = sheet_rows(plan, sheet, 0, 2 * plan.tall)
            return carry

        lax.fori_loop(0, groups, turn, 0)
        over_a.finish(groups)
        over_b.finish(groups)


def middle_kernel(
    plan, modes, skip, pre, weights, weight, lift, t_plane, t_x, t_y, s_y, s_x, s_plane,
    result, values, wide, field, sheet, real_first, imag_first, folded, real_sum, imag_sum,
    *scratch,
):
    step = pl.program_id(0)
    back_a, back_b = exchanges(plan, scratch[:8])
    over_a, over_b = exchanges(plan, scratch[8:16])
    last_a, last_b = exchanges(plan, scratch[16:])
    groups, group, tall = plan.groups, plan.group, plan.tall
    lanes = 512

    @pl.when(step == 0)
    def _():
        greet(plan)

        def send(index, carry):
            y_out(plan, index, (modes[index, :tall], modes[index, tall:]), s_y, back_b)
            return carry

        lax.fori_loop(0, groups, send, 0)
        result[...] = jnp.zeros_like(result)
        real_sum[...] = jnp.zeros_like(real_sum)
        imag_sum[...] = jnp.zeros_like(imag_sum)

    @pl.when(step < groups)
    def _():
        fold_in(plan, step, weights, lift, folded)
        x_out(plan, step, s_x, back_b, back_a)

    @pl.when(jnp.logical_and(step >= 1, step <= groups))
    def _():
        at = step - 1
        values[...] = plane_out(plan, at, group, s_plane, back_a)

        def line(index, carry):
            c = index // plan.xb
            x = index % plan.xb
            scale = weight[at * group + c]
            row = pl.multiple_of(index * plan.yb, plan.yb)
            spot = pl.multiple_of(x * plan.yb, plan.yb)
            for first in range(0, plan.cells, lanes):
                cut = pl.ds(first, lanes)
                slope = gelu_slope(pre[0, 0, c, x, :, cut].astype(F32))
                incoming = values[pl.ds(row, plan.yb), cut] + skip[c, x, :, cut].astype(F32)
                value = (incoming * slope).astype(BF16)
                field[pl.ds(row, plan.yb), cut] = value
                result[pl.ds(spot, plan.yb), cut] += value.astype(F32) * scale
            return carry

        lax.fori_loop(0, group * plan.xb, line, 0)
        plane_in(plan, at, field[...], t_plane, wide, over_a)

    @pl.when(jnp.logical_and(step >= 2, step <= groups + 1))
    def _():
        x_in(plan, step - 2, t_x, over_a, over_b)

    @pl.when(step >= 3)
    def _():
        at = step - 3
        y_in(plan, at, t_y, over_b, sheet, real_first, imag_first)
        for c in range(group):
            matrix = folded[at * group + c]
            real_sum[...] += matrix * real_first[c]
            imag_sum[...] += matrix * imag_first[c]

    @pl.when(step == groups + 2)
    def _():
        rows = []
        for k in range(plan.kb):
            row = [total[k, :1] + total[k, 1:] for total in (real_sum, imag_sum)]
            rows.append(jnp.concatenate(row, 0))
        by_row(plan, rows, sheet)
        mb = plan.mb
        parts = [sheet_rows(plan, sheet, p * mb, (p + 1) * mb) for p in range(2)]
        y_out(plan, 0, parts, s_y, last_b)
        x_out(plan, 0, s_x, last_b, last_a)
        result[...] += plane_out(plan, 0, 1, s_plane, last_a)
        for each in (back_a, back_b, over_a, over_b):
            each.finish(groups)
        for each in (last_a, last_b):
            each.finish(1)


def whole():
    return pl.BlockSpec(memory_space=pltpu.VMEM, pipeline_mode=pl.Buffered(1))


VMEM_LIMIT = 62 * 1024 * 1024


def weight_spec(plan, layer, first):
    block = (1, plan.group, plan.channels, plan.kb, 2, plan.lines)
    last = plan.groups - 1
    return pl.BlockSpec(block, lambda s: (layer, jnp.clip(s - first, 0, last), 0, 0, 0, 0))


def mixing_scratch(plan):
    line = (2, plan.lines)
    return [
        pltpu.VMEM((plan.room // 128, 2 * plan.tall, 128), F32),
        pltpu.VMEM((plan.group, plan.kb) + line, F32),
        pltpu.VMEM((plan.group, plan.kb) + line, F32),
    ]


def forward_call(plan, layer, cotangent, pre_activations, weights, tables, mix):
    groups, group = plan.groups, plan.group
    field = (plan.xb, plan.yb, plan.cells)
    sums = (plan.channels, plan.kb, 2, plan.lines)

    def at_group(step):
        return jnp.minimum(step, groups - 1)

    return pl.pallas_call(
        functools.partial(forward_kernel, plan),
        grid=(groups + 2,),
        in_specs=[
            pl.BlockSpec((1, group) + field, lambda s: (0, at_group(s), 0, 0, 0)),
            pl.BlockSpec((1, 1, group) + field, lambda s: (layer, 0, at_group(s), 0, 0, 0)),
            weight_spec(plan, layer, 2),
            whole(),
            whole(),
            whole(),
            whole(),
        ],
        out_specs=[
            pl.BlockSpec(
                (plan.channels, plan.xb // 2, plan.yb, plan.cells),
                lambda s: (0, jnp.clip(s - groups, 0, 1), 0, 0),
            ),
            pl.BlockSpec((groups, 2 * plan.tall, plan.modes), lambda s: (0, 0, 0)),
        ],
        out_shape=[
            jax.ShapeDtypeStruct((plan.channels,) + field, BF16),
            jax.ShapeDtypeStruct((groups, 2 * plan.tall, plan.modes), BF16),
        ],
        scratch_shapes=[
            pltpu.VMEM((plan.channels,) + field, BF16),
            pltpu.VMEM((2 * KZ * KT, group * plan.spots), F32),
        ]
        + mixing_scratch(plan)
        + [pltpu.VMEM(sums, F32), pltpu.VMEM(sums, F32)]
        + exchange_scratch(plan, groups, plan.tall),
        compiler_params=pltpu.CompilerParams(
            collective_id=1, has_side_effects=True, vmem_limit_bytes=VMEM_LIMIT
        ),
        name="forward",
    )(cotangent, pre_activations, weights, tables["plane_in"], tables["x_in"], tables["y_in"], mix)


def middle_call(plan, layer, modes, skip, pre_activations, weights, weight, lift, tables):
    groups, group = plan.groups, plan.group
    field = (plan.xb, plan.yb, plan.cells)
    sums = (plan.kb, 2, plan.lines)

    def at_group(step):
        return jnp.clip(step - 1, 0, groups - 1)

    names = ("plane_in", "x_in", "y_in", "y_out", "x_out", "plane_out")
    return pl.pallas_call(
        functools.partial(middle_kernel, plan),
        grid=(groups + 3,),
        in_specs=[
            whole(),
            pl.BlockSpec((group,) + field, lambda s: (at_group(s), 0, 0, 0)),
            pl.BlockSpec((1, 1, group) + field, lambda s: (layer, 0, at_group(s), 0, 0, 0)),
            weight_spec(plan, layer, 0),
            pl.BlockSpec(memory_space=pltpu.SMEM),
            pl.BlockSpec(memory_space=pltpu.SMEM),
        ]
        + [whole()] * len(names),
        out_specs=pl.BlockSpec((plan.spots, plan.cells), lambda s: (0, 0)),
        out_shape=jax.ShapeDtypeStruct((plan.spots, plan.cells), F32),
        scratch_shapes=[
            pltpu.VMEM((group * plan.spots, plan.cells), F32),
            pltpu.VMEM((2 * KZ * KT, group * plan.spots), F32),
            pltpu.VMEM((group * plan.spots, plan.cells), BF16),
        ]
        + mixing_scratch(plan)
        + [pltpu.VMEM((plan.channels,) + sums, F32)]
        + [pltpu.VMEM(sums, F32), pltpu.VMEM(sums, F32)]
        + exchange_scratch(plan, groups, plan.tall)
        + exchange_scratch(plan, groups, plan.tall)
        + exchange_scratch(plan, 1, -(-plan.mb // 16) * 16),
        compiler_params=pltpu.CompilerParams(
            collective_id=2, has_side_effects=True, vmem_limit_bytes=VMEM_LIMIT
        ),
        name="middle",
    )(modes, skip, pre_activations, weights, weight, lift, *[tables[name] for name in names])


def per_device(plan, cotangent, pre_activations, spectral_weights, skip_weights, lift_weights):
    tables = dense_tables(plan)
    weights = spectral_weights.transpose(0, 2, 3, 4, 1, 5)
    mix = jnp.kron(skip_weights[1].T, jnp.eye(plan.yb, dtype=BF16))
    weight = jnp.sum(skip_weights[0].astype(F32) * lift_weights[None, :], 1)
    skip, modes = forward_call(plan, 1, cotangent, pre_activations, weights, tables, mix)
    result = middle_call(
        plan, 0, modes, skip, pre_activations, weights, weight, lift_weights, tables
    )
    return result.reshape(1, plan.xb, plan.yb, plan.cells)


def solution(mesh):
    def step(cotangent, pre_activations, spectral_weights, skip_weights, lift_weights):
        plan = Plan(mesh, cotangent.shape[1])
        layers, samples = pre_activations.shape[:2]
        if layers == 2 and samples == 1 and plan.fits():
            body = functools.partial(per_device, plan)
        else:
            body = per_device_plain
        return body(cotangent, pre_activations, spectral_weights, skip_weights, lift_weights)

    return jax.shard_map(
        step,
        mesh=mesh,
        in_specs=(
            P(None, None, "aa", "ba", None),
            P(None, None, None, "aa", "ba", None),
            P(None, None, None, None, "ba", "aa"),
            P(),
            P(),
        ),
        out_specs=P(None, "aa", "ba", None),
        check_vma=False,
    )
```

```python
import functools
import math

import jax
import jax.numpy as jnp
import numpy as np
from jax import lax
from jax.experimental import pallas as pl
from jax.experimental.pallas import tpu as pltpu
from jax.sharding import PartitionSpec as P

NX = 64
NY = 64
NZ = 64
NT = 32
KX = 24
KY = 24
KZ = 24
KT = 12


def gelu_slope(values):
    normal_cdf = 0.5 * (1.0 + lax.erf(values / math.sqrt(2.0)))
    density = jnp.exp(-0.5 * values * values) / math.sqrt(2.0 * math.pi)
    return normal_cdf + values * density


def signed_freq(total_count):
    index_list = np.arange(total_count)
    return np.where(index_list < total_count // 2, index_list, index_list - total_count)


def line_tables(total_count, length):
    turns = signed_freq(total_count)[:, None] * np.arange(length)[None, :] % length
    angles = 2.0 * math.pi / length * turns
    cosine = np.cos(angles)
    sine_part = np.sin(angles)
    forward = np.stack(
        [np.stack([cosine.T, -sine_part.T], 1), np.stack([sine_part.T, cosine.T], 1)], 0
    )
    inverse = (
        np.stack([np.stack([cosine, sine_part], 1), np.stack([-sine_part, cosine], 1)], 0)
        / length
    )
    return (forward, inverse)


def plane_tables():
    joint_index = np.arange(KZ * KT)
    depth_freq = signed_freq(KZ)[joint_index // KT]
    time_freq = joint_index % KT
    cell_index = np.arange(NZ * NT)
    turns = (
        depth_freq[:, None] * (cell_index // NT)[None, :] * NT
        + time_freq[:, None] * (cell_index % NT)[None, :] * NZ
    ) % (NZ * NT)
    angles = 2.0 * math.pi / (NZ * NT) * turns
    forward = np.stack([np.cos(angles).T, -np.sin(angles).T], 1)
    inverse = np.stack([np.cos(angles), -np.sin(angles)], 0) / (NZ * NT)
    return (forward, inverse)


def rounded_product(pattern, values, table):
    return jnp.einsum(
        pattern, values, jnp.asarray(table, jnp.bfloat16), preferred_element_type=jnp.float32
    )


def exact_product(pattern, values, table):
    return jnp.einsum(
        pattern, values, jnp.asarray(table, jnp.float32), precision=lax.Precision.HIGHEST
    )


def to_bf16(values):
    return values.astype(jnp.bfloat16)


def keep_float(values):
    return values


def exchange(values, axis):
    return lax.all_to_all(values, axis, split_axis=0, concat_axis=0, tiled=True)


def forward_modes(grad_pre, weights, tables):
    plane, first, second = tables
    rows = lax.axis_size("aa")
    columns = lax.axis_size("ba")
    plane = plane.reshape(NZ * NT, 2, rows, -1)
    spectrum = to_bf16(rounded_product("bcxyz,zpnm->nbcpxmy", grad_pre, plane))
    blocks = exchange(spectrum, "aa")
    first = first.reshape(2, rows, NX // rows, 2, columns, KX // columns)
    spectrum = to_bf16(rounded_product("nbcpxmy,pnxqgk->gbcqkmy", blocks, first))
    blocks = exchange(spectrum, "ba")
    second = second.reshape(2, columns, NY // columns, 2, KY)
    result = to_bf16(rounded_product("gbcpkmy,pgyqj->bcqkmj", blocks, second))
    shape = result.shape
    spectrum = result.reshape(shape[:4] + (shape[4] * KY,))
    real_part = spectrum[:, :, 0]
    imag_part = spectrum[:, :, 1]

    def mixing(values, matrix):
        return jnp.einsum("bokr,oikr->bikr", values, matrix, preferred_element_type=jnp.float32)

    result_real = mixing(real_part, weights[0]) + mixing(imag_part, weights[1])
    result_imag = mixing(imag_part, weights[0]) - mixing(real_part, weights[1])
    return jnp.stack([result_real, result_imag], 2)


def back_path(mode_values, tables, multiply, finish):
    first, second, plane = tables
    rows = lax.axis_size("aa")
    columns = lax.axis_size("ba")
    extent = mode_values.shape
    gridded = mode_values.reshape(extent[:4] + (extent[4] // KY, KY))
    second = second.reshape(2, KY, 2, columns, NY // columns)
    blocks = exchange(finish(multiply("bcpkmj,pjqgu->gbcqkmu", gridded, second)), "ba")
    first = first.reshape(2, columns, KX // columns, 2, rows, NX // rows)
    back = to_bf16(multiply("gbcpkmu,pgkqnx->nbcqxmu", blocks, first))
    blocks = exchange(back, "aa")
    plane = plane.reshape(2, rows, -1, NZ * NT)
    return rounded_product("nbcpxmu,pnmz->bcxuz", blocks, plane)


def per_device_plain(cotangent, pre_activations, spectral_weights, skip_weights, lift_weights):
    plane_forward, plane_inverse = plane_tables()
    first_forward, first_inverse = line_tables(KX, NX)
    second_forward, second_inverse = line_tables(KY, NY)
    forward_tables = (plane_forward, first_forward, second_forward)
    back_tables = (first_inverse, second_inverse, plane_inverse)
    incoming = cotangent.astype(jnp.float32)
    layers = pre_activations.shape[0]
    perm_grad = None
    for layer_index in range(layers - 1, -1, -1):
        slope = gelu_slope(pre_activations[layer_index].astype(jnp.float32))
        grad_pre = (incoming * slope).astype(jnp.bfloat16)
        mode_values = forward_modes(grad_pre, spectral_weights[layer_index], forward_tables)
        if layer_index > 0:
            skip_term = jnp.einsum(
                "boxyz,oi->bixyz",
                grad_pre,
                skip_weights[layer_index],
                preferred_element_type=jnp.float32,
            )
            spectral = back_path(
                mode_values.astype(jnp.bfloat16), back_tables, rounded_product, to_bf16
            )
            incoming = skip_term + spectral
        else:
            folded = jnp.sum(mode_values * lift_weights[None, :, None, None, None], 1)[:, None]
            spectral = back_path(folded, back_tables, exact_product, keep_float)
            combined = jnp.sum(skip_weights[0].astype(jnp.float32) * lift_weights[None, :], 1)
            projected = jnp.sum(
                grad_pre.astype(jnp.float32) * combined[None, :, None, None, None], 1
            )
            perm_grad = projected + spectral[:, 0]
    return perm_grad


F32 = jnp.float32
BF16 = jnp.bfloat16
MESH = pl.DeviceIdType.MESH


class Plan:
    def __init__(self, mesh, channels):
        self.rows = mesh.shape["aa"]
        self.columns = mesh.shape["ba"]
        self.xb = NX // self.rows
        self.yb = NY // self.columns
        self.mb = KZ * KT // self.rows
        self.kb = KX // self.columns
        self.cells = NZ * NT
        self.spots = self.xb * self.yb
        self.channels = channels
        self.group = 4
        self.groups = channels // self.group
        self.tall = self.group * self.mb
        self.half = 128
        self.kmain = self.half // (2 * self.yb)
        self.width = 2 * self.kb * self.yb
        self.modes = self.kb * KY
        self.room = -(-self.modes // 128) * 128
        self.lines = self.mb * KY

    def fits(self):
        return (
            self.spots == self.half
            and self.half % self.yb == 0
            and self.yb % 16 == 0
            and self.half % (2 * self.yb) == 0
            and 2 * (self.width - self.half) == self.half
            and self.columns % 2 == 0
            and self.channels % self.group == 0
            and self.tall % 16 == 0
            and self.xb % 2 == 0
        )


def real_form(matrix):
    top = np.stack([matrix.real, matrix.imag], 1)
    low = np.stack([-matrix.imag, matrix.real], 1)
    return np.stack([top, low], 0)


def line_phase(count, length):
    turns = signed_freq(count)[:, None] * np.arange(length)[None, :] % length
    return np.exp(2j * math.pi * turns / length)


def dense_tables(plan):
    rows, columns = plan.rows, plan.columns
    eye_y = np.eye(plan.yb)
    eye_k = np.eye(plan.kb)
    along_x = line_phase(KX, NX)
    along_y = line_phase(KY, NY)
    plane_forward, plane_inverse = plane_tables()
    tables = {}

    def split(wide, axis):
        main, left = np.split(wide, [plan.kmain], axis + 1)
        shape = wide.shape[:axis] + (-1,) + wide.shape[axis + 4 :]
        return np.concatenate([main.reshape(shape), left.reshape(shape)], axis)

    tables["plane_in"] = plane_forward.transpose(1, 2, 0).reshape(2 * KZ * KT, plan.cells)
    part = real_form(along_x.conj().T).reshape(2, rows, plan.xb, 2, columns, plan.kb)
    wide = np.einsum("psxqgk,yw->spxygkqw", part, eye_y)
    wide = wide.reshape((rows * 2 * plan.spots,) + wide.shape[4:])
    tables["x_in"] = split(wide, 1)
    part = real_form(along_y.conj().T).reshape(2, columns, plan.yb, 2, KY)
    wide = split(np.einsum("pbyqj,kl->blpyqkj", part, eye_k), 0)
    wide = wide.reshape(columns * plan.width, 2, plan.modes)
    wide = np.pad(wide, ((0, 0), (0, 0), (0, plan.room - plan.modes)))
    tables["y_in"] = wide.reshape(columns * plan.width, 2 * plan.room)
    part = (real_form(along_y) / NY).reshape(2, KY, 2, columns, plan.yb)
    wide = split(np.einsum("pjqhy,kl->pkjhlqy", part, eye_k), 3)
    tables["y_out"] = wide.reshape(2, plan.modes, columns * plan.width)
    part = (real_form(along_x) / NX).reshape(2, columns, plan.kb, 2, rows, plan.xb)
    wide = split(np.einsum("pbkqnx,yw->bkpynqxw", part, eye_y), 0)
    tables["x_out"] = wide.reshape(columns * plan.width, rows * 2 * plan.spots)
    back = plane_inverse.reshape(2, rows, plan.mb, plan.cells).transpose(1, 0, 2, 3)
    tables["plane_out"] = back.reshape(2 * KZ * KT, plan.cells)
    return {name: jnp.asarray(table.astype(jnp.bfloat16)) for name, table in tables.items()}


def slope_twice(values):
    scaled = values * math.sqrt(0.5)
    bell = jnp.exp2(scaled * scaled * -math.log2(math.e))
    return 1.0 + lax.erf(scaled) + scaled * (2.0 / math.sqrt(math.pi)) * bell


def product(left, right, contract=((1,), (0,))):
    return lax.dot_general(left, right, (contract, ((), ())), preferred_element_type=F32)


def greet(plan):
    barrier = pltpu.get_barrier_semaphore()
    for axis, size in (("aa", plan.rows), ("ba", plan.columns)):
        for hop in range(1, size):
            peer = lax.rem(lax.axis_index(axis) + hop, size)
            pl.semaphore_signal(barrier, inc=1, device_id={axis: peer}, device_id_type=MESH)
    pl.semaphore_wait(barrier, plan.rows + plan.columns - 2)


class Tables:
    def __init__(self, sources, places, sems):
        self.sources, self.places, self.sems = sources, places, sems

    def copy(self, index):
        return pltpu.make_async_copy(self.sources[index], self.places[index], self.sems.at[index])

    def start(self):
        for index in range(len(self.sources)):
            self.copy(index).start()


class Exchange:
    def __init__(self, axis, size, out, into, sent, came):
        self.axis, self.size = axis, size
        self.out, self.into, self.sent, self.came = out, into, sent, came

    def copy(self, group, hop):
        me = lax.axis_index(self.axis)
        peer = lax.rem(me + hop, self.size)
        return pltpu.make_async_remote_copy(
            src_ref=self.out.at[group, peer],
            dst_ref=self.into.at[group, me],
            send_sem=self.sent.at[group, hop],
            recv_sem=self.came.at[group, hop],
            device_id={self.axis: peer},
            device_id_type=MESH,
        )

    def start(self, group):
        for hop in range(1, self.size):
            self.copy(group, hop).start()
        me = lax.axis_index(self.axis)
        self.into[group, me] = self.out[group, me]

    def arrive(self, group):
        for hop in range(1, self.size):
            self.copy(group, hop).wait_recv()

    def finish(self, groups):
        def drain(group, carry):
            for hop in range(1, self.size):
                self.copy(group, hop).wait_send()
            return carry

        lax.fori_loop(0, groups, drain, 0)


def exchange_scratch(plan, groups, tall):
    rows, columns = plan.rows, plan.columns
    return [
        pltpu.VMEM((groups, rows, tall, 2 * plan.spots), BF16),
        pltpu.VMEM((groups, rows, tall, 2 * plan.spots), BF16),
        pltpu.SemaphoreType.DMA((groups, rows)),
        pltpu.SemaphoreType.DMA((groups, rows)),
        pltpu.VMEM((groups, columns, tall + tall // 2, plan.half), BF16),
        pltpu.VMEM((groups, columns, tall + tall // 2, plan.half), BF16),
        pltpu.SemaphoreType.DMA((groups, columns)),
        pltpu.SemaphoreType.DMA((groups, columns)),
    ]


def exchanges(plan, scratch):
    return (
        Exchange("aa", plan.rows, *scratch[:4]),
        Exchange("ba", plan.columns, *scratch[4:8]),
    )


def plane_in(plan, group, values, table, wide, over_a):
    rows, mb, spots = plan.rows, plan.mb, plan.spots
    wide[...] = product(table[...], values, ((1,), (1,)))
    for owner in range(rows):
        halves = []
        for part in range(2):
            first = (part * rows + owner) * mb
            halves.append(
                jnp.concatenate(
                    [
                        wide[first : first + mb, c * spots : (c + 1) * spots]
                        for c in range(plan.group)
                    ],
                    0,
                )
            )
        over_a.out[group, owner] = jnp.concatenate(halves, 1).astype(BF16)
    over_a.start(group)


def joined(ref, group, size):
    return jnp.concatenate([ref[group, index] for index in range(size)], 1)


def low_lanes(rows, half):
    return lax.broadcasted_iota(jnp.int32, (rows, half), 1) < half // 2


def pack(plan, group, values, over_b):
    half = plan.half
    tall = values.shape[0]
    low = low_lanes(tall // 2, half)
    for pair in range(plan.columns // 2):
        first = (plan.columns + pair) * half
        left = values[:, first : first + half]
        turned = pltpu.roll(left, half // 2, 1)
        for side, (upper, lower) in enumerate(((left, turned), (turned, left))):
            owner = 2 * pair + side
            main = values[:, owner * half : (owner + 1) * half]
            rest = jnp.where(low, upper[: tall // 2], lower[tall // 2 :])
            over_b.out[group, owner] = jnp.concatenate([main, rest], 0).astype(BF16)
    over_b.start(group)


def unpack(plan, group, over_b):
    over_b.arrive(group)
    half = plan.half
    tall = over_b.into.shape[2] * 2 // 3
    low = low_lanes(tall // 2, half)
    mains = [over_b.into[group, index, :tall] for index in range(plan.columns)]
    for pair in range(plan.columns // 2):
        first, second = [over_b.into[group, 2 * pair + side, tall:].astype(F32) for side in (0, 1)]
        upper = jnp.where(low, first, pltpu.roll(second, half // 2, 1))
        lower = jnp.where(low, pltpu.roll(first, half // 2, 1), second)
        mains.append(jnp.concatenate([upper, lower], 0).astype(BF16))
    return jnp.concatenate(mains, 1)


def x_in(plan, group, table, over_a, over_b):
    over_a.arrive(group)
    result = product(joined(over_a.into, group, plan.rows), table[...])
    pack(plan, group, result, over_b)


def y_in(plan, group, table, over_b, sheet, real_first, imag_first):
    result = product(unpack(plan, group, over_b), table[...])
    mb = plan.mb
    for c in range(plan.group):
        for part in range(2):
            lane = part * plan.room
            row = (2 * c + part) * mb
            for half in range(plan.room // 128):
                first = lane + 128 * half
                piece = result[c * mb : (c + 1) * mb, first : first + 128]
                sheet[half, row : row + mb] = piece
    count = 2 * plan.group
    lines = []
    for m in range(mb):
        row = pl.ds(m, count, stride=mb)
        lines.append(jnp.concatenate([sheet[h, row, :] for h in range(plan.room // 128)], 1))
    for k in range(plan.kb):
        turned = jnp.concatenate([line[:, k * KY : (k + 1) * KY] for line in lines], 1)
        for c in range(plan.group):
            real = turned[2 * c : 2 * c + 1]
            imag = turned[2 * c + 1 : 2 * c + 2]
            real_first[c, k] = jnp.concatenate([real, imag], 0)
            imag_first[c, k] = jnp.concatenate([imag, -real], 0)


def mix_in(plan, weights, real_first, imag_first, real_sum, imag_sum):
    for c in range(plan.group):
        for k in range(plan.kb):
            first = real_first[c, k]
            second = imag_first[c, k]

            def add(i, carry):
                matrix = weights[0, c, i, k].astype(F32)
                real_sum[i, k] += matrix * first
                imag_sum[i, k] += matrix * second
                return carry

            lax.fori_loop(0, plan.channels, add, 0, unroll=10)


def fold_in(plan, group, weights, lift, folded):
    for c in range(plan.group):

        def line(k, carry):
            total = weights[0, c, 0, k].astype(F32) * lift[0]
            for i in range(1, plan.channels):
                total = total + weights[0, c, i, k].astype(F32) * lift[i]
            folded[group * plan.group + c, k] = total
            return carry

        lax.fori_loop(0, plan.kb, line, 0)


def by_row(plan, rows, sheet):
    count = rows[0].shape[0]
    for m in range(plan.mb):
        pieces = [row[:, m * KY : (m + 1) * KY] for row in rows]
        if plan.room > plan.modes:
            pieces.append(jnp.zeros((count, plan.room - plan.modes), F32))
        line = jnp.concatenate(pieces, 1)
        for half in range(plan.room // 128):
            row = pl.ds(m, count, stride=plan.mb)
            sheet[half, row, :] = line[:, half * 128 : (half + 1) * 128]


def sheet_rows(plan, sheet, first, last):
    halves = [sheet[half, first:last] for half in range(plan.room // 128)]
    return jnp.concatenate(halves, 1)[:, : plan.modes].astype(BF16)


def y_out(plan, group, parts, table, over_b):
    result = product(parts[0], table[0]) + product(parts[1], table[1])
    tall = over_b.out.shape[2] * 2 // 3
    if result.shape[0] < tall:
        more = jnp.zeros((tall - result.shape[0], result.shape[1]), F32)
        result = jnp.concatenate([result, more], 0)
    pack(plan, group, result, over_b)


def x_out(plan, group, table, over_b, over_a):
    values = unpack(plan, group, over_b)
    width = 2 * plan.spots
    for owner in range(plan.rows):
        cut = table[:, owner * width : (owner + 1) * width]
        over_a.out[group, owner] = product(values, cut).astype(BF16)
    over_a.start(group)


def plane_out(plan, group, count, table, over_a):
    over_a.arrive(group)
    mb, spots = plan.mb, plan.spots
    pieces = []
    for source in range(plan.rows):
        block = over_a.into[group, source].astype(F32)
        for part in range(2):
            pieces.append(
                jnp.concatenate(
                    [
                        block[c * mb : (c + 1) * mb, part * spots : (part + 1) * spots]
                        for c in range(count)
                    ],
                    1,
                )
            )
    values = jnp.concatenate(pieces, 0).astype(BF16)
    return product(values, table[...], ((0,), (0,)))


def forward_kernel(
    plan, cotangent, pre, weights, h_plane, h_x, h_y, mix, skip, modes,
    t_plane, t_x, t_y, table_sems, field, wide, sheet, real_first, imag_first, real_sum, imag_sum, *scratch,
):
    step = pl.program_id(0)
    over_a, over_b = exchanges(plan, scratch)
    groups, group = plan.groups, plan.group
    lanes = 512
    tables = Tables((h_plane, h_x, h_y), (t_plane, t_x, t_y), table_sems)

    @pl.when(step == 0)
    def _():
        tables.start()
        greet(plan)
        real_sum[...] = jnp.zeros_like(real_sum)
        imag_sum[...] = jnp.zeros_like(imag_sum)

    @pl.when(step < groups)
    def _():
        def line(index, carry):
            c = index // plan.xb
            x = index % plan.xb
            for first in range(0, plan.cells, lanes):
                cut = pl.ds(first, lanes)
                slope = slope_twice(pre[0, 0, c, x, :, cut].astype(F32))
                value = cotangent[0, c, x, :, cut].astype(F32) * 0.5 * slope
                field[step * group + c, x, :, cut] = value.astype(BF16)
            return carry

        lax.fori_loop(0, group * plan.xb, line, 0, unroll=2)

        @pl.when(step == 0)
        def _():
            tables.copy(0).wait()

        values = field[pl.ds(step * group, group)].reshape(group * plan.spots, plan.cells)
        plane_in(plan, step, values, t_plane, wide, over_a)

    @pl.when(step >= groups)
    def _():
        def line(index, carry):
            x = (step - groups) * (plan.xb // 2) + index
            tile = plan.yb // 2
            for first in range(0, plan.cells, lanes):
                cut = pl.ds(first, lanes)
                for y in (pl.ds(0, tile), pl.ds(tile, tile)):
                    values = field[:, x, y, cut].reshape(plan.channels * tile, lanes)
                    result = product(mix[...], values).astype(BF16)
                    skip[:, index, y, cut] = result.reshape(plan.channels, tile, lanes)
            return carry

        lax.fori_loop(0, plan.xb // 2, line, 0)

    @pl.when(step == 1)
    def _():
        tables.copy(1).wait()

    @pl.when(jnp.logical_and(step >= 1, step <= groups))
    def _():
        x_in(plan, step - 1, t_x, over_a, over_b)

    @pl.when(step == 2)
    def _():
        tables.copy(2).wait()

    @pl.when(step >= 2)
    def _():
        y_in(plan, step - 2, t_y, over_b, sheet, real_first, imag_first)
        mix_in(plan, weights, real_first, imag_first, real_sum, imag_sum)

    @pl.when(step == groups + 1)
    def _():
        def turn(index, carry):
            rows = []
            for k in range(plan.kb):
                row = []
                for total in (real_sum, imag_sum):
                    for c in range(group):
                        both = total[index * group + c, k]
                        row.append(both[:1] + both[1:])
                rows.append(jnp.concatenate(row, 0))
            by_row(plan, rows, sheet)
            modes[index] = sheet_rows(plan, sheet, 0, 2 * plan.tall)
            return carry

        lax.fori_loop(0, groups, turn, 0)
        over_a.finish(groups)
        over_b.finish(groups)


def middle_kernel(
    plan, modes, skip, pre, weights, weight, lift, *refs,
):
    (h_s_y, h_s_x, h_s_plane, h_plane, h_x, h_y, result) = refs[:7]
    (s_y, s_x, s_plane, t_plane, t_x, t_y, table_sems) = refs[7:14]
    (values, wide, field, sheet, real_first, imag_first, folded) = refs[14:21]
    (real_sum, imag_sum), scratch = refs[21:23], refs[23:]
    step = pl.program_id(0)
    back_a, back_b = exchanges(plan, scratch[:8])
    over_a, over_b = exchanges(plan, scratch[8:16])
    last_a, last_b = exchanges(plan, scratch[16:])
    groups, group, tall = plan.groups, plan.group, plan.tall
    lanes = 512
    sources = (h_s_y, h_s_x, h_s_plane, h_plane, h_x, h_y)
    tables = Tables(sources, (s_y, s_x, s_plane, t_plane, t_x, t_y), table_sems)

    @pl.when(step == 0)
    def _():
        tables.start()
        greet(plan)
        tables.copy(0).wait()

        def send(index, carry):
            y_out(plan, index, (modes[index, :tall], modes[index, tall:]), s_y, back_b)
            return carry

        lax.fori_loop(0, groups, send, 0)
        result[...] = jnp.zeros_like(result)
        real_sum[...] = jnp.zeros_like(real_sum)
        imag_sum[...] = jnp.zeros_like(imag_sum)
        tables.copy(1).wait()

    def ahead(at, carry):
        x_out(plan, at, s_x, back_b, back_a)
        return carry

    first = jnp.where(step == 0, 0, jnp.minimum(step + 1, groups))
    lax.fori_loop(first, jnp.minimum(step + 2, groups), ahead, 0)

    @pl.when(step == 0)
    def _():
        for index in range(2, 6):
            tables.copy(index).wait()

    @pl.when(step < groups)
    def _():
        fold_in(plan, step, weights, lift, folded)
        at = step
        values[...] = plane_out(plan, at, group, s_plane, back_a)

        def line(index, carry):
            c = index // plan.xb
            x = index % plan.xb
            scale = weight[at * group + c]
            row = pl.multiple_of(index * plan.yb, plan.yb)
            spot = pl.multiple_of(x * plan.yb, plan.yb)
            for first in range(0, plan.cells, lanes):
                cut = pl.ds(first, lanes)
                slope = 0.5 * slope_twice(pre[0, 0, c, x, :, cut].astype(F32))
                incoming = values[pl.ds(row, plan.yb), cut] + skip[c, x, :, cut].astype(F32)
                value = (incoming * slope).astype(BF16)
                field[pl.ds(row, plan.yb), cut] = value
                result[pl.ds(spot, plan.yb), cut] += value.astype(F32) * scale
            return carry

        lax.fori_loop(0, group * plan.xb, line, 0, unroll=2)
        plane_in(plan, at, field[...], t_plane, wide, over_a)

    @pl.when(jnp.logical_and(step >= 1, step <= groups))
    def _():
        x_in(plan, step - 1, t_x, over_a, over_b)

    @pl.when(step >= 2)
    def _():
        at = step - 2
        y_in(plan, at, t_y, over_b, sheet, real_first, imag_first)
        for c in range(group):
            matrix = folded[at * group + c]
            real_sum[...] += matrix * real_first[c]
            imag_sum[...] += matrix * imag_first[c]

    @pl.when(step == groups + 1)
    def _():
        rows = []
        for k in range(plan.kb):
            row = [total[k, :1] + total[k, 1:] for total in (real_sum, imag_sum)]
            rows.append(jnp.concatenate(row, 0))
        by_row(plan, rows, sheet)
        mb = plan.mb
        parts = [sheet_rows(plan, sheet, p * mb, (p + 1) * mb) for p in range(2)]
        y_out(plan, 0, parts, s_y, last_b)
        x_out(plan, 0, s_x, last_b, last_a)
        result[...] += plane_out(plan, 0, 1, s_plane, last_a)
        for each in (back_a, back_b, over_a, over_b):
            each.finish(groups)
        for each in (last_a, last_b):
            each.finish(1)


def whole():
    return pl.BlockSpec(memory_space=pltpu.VMEM, pipeline_mode=pl.Buffered(1))


VMEM_LIMIT = 62 * 1024 * 1024


def weight_spec(plan, layer, first):
    block = (1, plan.group, plan.channels, plan.kb, 2, plan.lines)
    last = plan.groups - 1
    return pl.BlockSpec(block, lambda s: (layer, jnp.clip(s - first, 0, last), 0, 0, 0, 0))


def table_scratch(tables, names):
    places = [pltpu.VMEM(tables[name].shape, BF16) for name in names]
    return places + [pltpu.SemaphoreType.DMA((len(names),))]


def mixing_scratch(plan):
    line = (2, plan.lines)
    return [
        pltpu.VMEM((plan.room // 128, 2 * plan.tall, 128), F32),
        pltpu.VMEM((plan.group, plan.kb) + line, F32),
        pltpu.VMEM((plan.group, plan.kb) + line, F32),
    ]


def forward_call(plan, layer, cotangent, pre_activations, weights, tables, mix):
    groups, group = plan.groups, plan.group
    field = (plan.xb, plan.yb, plan.cells)
    sums = (plan.channels, plan.kb, 2, plan.lines)

    def at_group(step):
        return jnp.minimum(step, groups - 1)

    return pl.pallas_call(
        functools.partial(forward_kernel, plan),
        grid=(groups + 2,),
        in_specs=[
            pl.BlockSpec((1, group) + field, lambda s: (0, at_group(s), 0, 0, 0)),
            pl.BlockSpec((1, 1, group) + field, lambda s: (layer, 0, at_group(s), 0, 0, 0)),
            weight_spec(plan, layer, 2),
            pl.BlockSpec(memory_space=pl.ANY),
            pl.BlockSpec(memory_space=pl.ANY),
            pl.BlockSpec(memory_space=pl.ANY),
            whole(),
        ],
        out_specs=[
            pl.BlockSpec(
                (plan.channels, plan.xb // 2, plan.yb, plan.cells),
                lambda s: (0, jnp.clip(s - groups, 0, 1), 0, 0),
            ),
            pl.BlockSpec((groups, 2 * plan.tall, plan.modes), lambda s: (0, 0, 0)),
        ],
        out_shape=[
            jax.ShapeDtypeStruct((plan.channels,) + field, BF16),
            jax.ShapeDtypeStruct((groups, 2 * plan.tall, plan.modes), BF16),
        ],
        scratch_shapes=table_scratch(tables, ("plane_in", "x_in", "y_in"))
        + [
            pltpu.VMEM((plan.channels,) + field, BF16),
            pltpu.VMEM((2 * KZ * KT, group * plan.spots), F32),
        ]
        + mixing_scratch(plan)
        + [pltpu.VMEM(sums, F32), pltpu.VMEM(sums, F32)]
        + exchange_scratch(plan, groups, plan.tall),
        compiler_params=pltpu.CompilerParams(
            collective_id=1, has_side_effects=True, vmem_limit_bytes=VMEM_LIMIT
        ),
        name="forward",
    )(cotangent, pre_activations, weights, tables["plane_in"], tables["x_in"], tables["y_in"], mix)


def middle_call(plan, layer, modes, skip, pre_activations, weights, weight, lift, tables):
    groups, group = plan.groups, plan.group
    field = (plan.xb, plan.yb, plan.cells)
    sums = (plan.kb, 2, plan.lines)

    def at_group(step):
        return jnp.minimum(step, groups - 1)

    names = ("y_out", "x_out", "plane_out", "plane_in", "x_in", "y_in")
    return pl.pallas_call(
        functools.partial(middle_kernel, plan),
        grid=(groups + 2,),
        in_specs=[
            whole(),
            pl.BlockSpec((group,) + field, lambda s: (at_group(s), 0, 0, 0)),
            pl.BlockSpec((1, 1, group) + field, lambda s: (layer, 0, at_group(s), 0, 0, 0)),
            weight_spec(plan, layer, 0),
            pl.BlockSpec(memory_space=pltpu.SMEM),
            pl.BlockSpec(memory_space=pltpu.SMEM),
        ]
        + [pl.BlockSpec(memory_space=pl.ANY)] * len(names),
        out_specs=pl.BlockSpec((plan.spots, plan.cells), lambda s: (0, 0)),
        out_shape=jax.ShapeDtypeStruct((plan.spots, plan.cells), F32),
        scratch_shapes=table_scratch(tables, names)
        + [
            pltpu.VMEM((group * plan.spots, plan.cells), F32),
            pltpu.VMEM((2 * KZ * KT, group * plan.spots), F32),
            pltpu.VMEM((group * plan.spots, plan.cells), BF16),
        ]
        + mixing_scratch(plan)
        + [pltpu.VMEM((plan.channels,) + sums, F32)]
        + [pltpu.VMEM(sums, F32), pltpu.VMEM(sums, F32)]
        + exchange_scratch(plan, groups, plan.tall)
        + exchange_scratch(plan, groups, plan.tall)
        + exchange_scratch(plan, 1, -(-plan.mb // 16) * 16),
        compiler_params=pltpu.CompilerParams(
            collective_id=2, has_side_effects=True, vmem_limit_bytes=VMEM_LIMIT
        ),
        name="middle",
    )(modes, skip, pre_activations, weights, weight, lift, *[tables[name] for name in names])


def per_device(plan, cotangent, pre_activations, spectral_weights, skip_weights, lift_weights):
    tables = dense_tables(plan)
    weights = spectral_weights.transpose(0, 2, 3, 4, 1, 5)
    mix = jnp.kron(skip_weights[1].T, jnp.eye(plan.yb // 2, dtype=BF16))
    weight = jnp.sum(skip_weights[0].astype(F32) * lift_weights[None, :], 1)
    skip, modes = forward_call(plan, 1, cotangent, pre_activations, weights, tables, mix)
    result = middle_call(
        plan, 0, modes, skip, pre_activations, weights, weight, lift_weights, tables
    )
    return result.reshape(1, plan.xb, plan.yb, plan.cells)


def solution(mesh):
    def step(cotangent, pre_activations, spectral_weights, skip_weights, lift_weights):
        plan = Plan(mesh, cotangent.shape[1])
        layers, samples = pre_activations.shape[:2]
        if layers == 2 and samples == 1 and plan.fits():
            body = functools.partial(per_device, plan)
        else:
            body = per_device_plain
        return body(cotangent, pre_activations, spectral_weights, skip_weights, lift_weights)

    return jax.shard_map(
        step,
        mesh=mesh,
        in_specs=(
            P(None, None, "aa", "ba", None),
            P(None, None, None, "aa", "ba", None),
            P(None, None, None, None, "ba", "aa"),
            P(),
            P(),
        ),
        out_specs=P(None, "aa", "ba", None),
        check_vma=False,
    )
```

```python
import functools
import math

import jax
import jax.numpy as jnp
import numpy as np
from jax import lax
from jax.experimental import pallas as pl
from jax.experimental.pallas import tpu as pltpu
from jax.sharding import PartitionSpec as P

NX = 64
NY = 64
NZ = 64
NT = 32
KX = 24
KY = 24
KZ = 24
KT = 12


def gelu_slope(values):
    normal_cdf = 0.5 * (1.0 + lax.erf(values / math.sqrt(2.0)))
    density = jnp.exp(-0.5 * values * values) / math.sqrt(2.0 * math.pi)
    return normal_cdf + values * density


def signed_freq(total_count):
    index_list = np.arange(total_count)
    return np.where(index_list < total_count // 2, index_list, index_list - total_count)


def line_tables(total_count, length):
    turns = signed_freq(total_count)[:, None] * np.arange(length)[None, :] % length
    angles = 2.0 * math.pi / length * turns
    cosine = np.cos(angles)
    sine_part = np.sin(angles)
    forward = np.stack(
        [np.stack([cosine.T, -sine_part.T], 1), np.stack([sine_part.T, cosine.T], 1)], 0
    )
    inverse = (
        np.stack([np.stack([cosine, sine_part], 1), np.stack([-sine_part, cosine], 1)], 0)
        / length
    )
    return (forward, inverse)


def plane_tables():
    joint_index = np.arange(KZ * KT)
    depth_freq = signed_freq(KZ)[joint_index // KT]
    time_freq = joint_index % KT
    cell_index = np.arange(NZ * NT)
    turns = (
        depth_freq[:, None] * (cell_index // NT)[None, :] * NT
        + time_freq[:, None] * (cell_index % NT)[None, :] * NZ
    ) % (NZ * NT)
    angles = 2.0 * math.pi / (NZ * NT) * turns
    forward = np.stack([np.cos(angles).T, -np.sin(angles).T], 1)
    inverse = np.stack([np.cos(angles), -np.sin(angles)], 0) / (NZ * NT)
    return (forward, inverse)


def rounded_product(pattern, values, table):
    return jnp.einsum(
        pattern, values, jnp.asarray(table, jnp.bfloat16), preferred_element_type=jnp.float32
    )


def exact_product(pattern, values, table):
    return jnp.einsum(
        pattern, values, jnp.asarray(table, jnp.float32), precision=lax.Precision.HIGHEST
    )


def to_bf16(values):
    return values.astype(jnp.bfloat16)


def keep_float(values):
    return values


def exchange(values, axis):
    return lax.all_to_all(values, axis, split_axis=0, concat_axis=0, tiled=True)


def forward_modes(grad_pre, weights, tables):
    plane, first, second = tables
    rows = lax.axis_size("aa")
    columns = lax.axis_size("ba")
    plane = plane.reshape(NZ * NT, 2, rows, -1)
    spectrum = to_bf16(rounded_product("bcxyz,zpnm->nbcpxmy", grad_pre, plane))
    blocks = exchange(spectrum, "aa")
    first = first.reshape(2, rows, NX // rows, 2, columns, KX // columns)
    spectrum = to_bf16(rounded_product("nbcpxmy,pnxqgk->gbcqkmy", blocks, first))
    blocks = exchange(spectrum, "ba")
    second = second.reshape(2, columns, NY // columns, 2, KY)
    result = to_bf16(rounded_product("gbcpkmy,pgyqj->bcqkmj", blocks, second))
    shape = result.shape
    spectrum = result.reshape(shape[:4] + (shape[4] * KY,))
    real_part = spectrum[:, :, 0]
    imag_part = spectrum[:, :, 1]

    def mixing(values, matrix):
        return jnp.einsum("bokr,oikr->bikr", values, matrix, preferred_element_type=jnp.float32)

    result_real = mixing(real_part, weights[0]) + mixing(imag_part, weights[1])
    result_imag = mixing(imag_part, weights[0]) - mixing(real_part, weights[1])
    return jnp.stack([result_real, result_imag], 2)


def back_path(mode_values, tables, multiply, finish):
    first, second, plane = tables
    rows = lax.axis_size("aa")
    columns = lax.axis_size("ba")
    extent = mode_values.shape
    gridded = mode_values.reshape(extent[:4] + (extent[4] // KY, KY))
    second = second.reshape(2, KY, 2, columns, NY // columns)
    blocks = exchange(finish(multiply("bcpkmj,pjqgu->gbcqkmu", gridded, second)), "ba")
    first = first.reshape(2, columns, KX // columns, 2, rows, NX // rows)
    back = to_bf16(multiply("gbcpkmu,pgkqnx->nbcqxmu", blocks, first))
    blocks = exchange(back, "aa")
    plane = plane.reshape(2, rows, -1, NZ * NT)
    return rounded_product("nbcpxmu,pnmz->bcxuz", blocks, plane)


def per_device_plain(cotangent, pre_activations, spectral_weights, skip_weights, lift_weights):
    plane_forward, plane_inverse = plane_tables()
    first_forward, first_inverse = line_tables(KX, NX)
    second_forward, second_inverse = line_tables(KY, NY)
    forward_tables = (plane_forward, first_forward, second_forward)
    back_tables = (first_inverse, second_inverse, plane_inverse)
    incoming = cotangent.astype(jnp.float32)
    layers = pre_activations.shape[0]
    perm_grad = None
    for layer_index in range(layers - 1, -1, -1):
        slope = gelu_slope(pre_activations[layer_index].astype(jnp.float32))
        grad_pre = (incoming * slope).astype(jnp.bfloat16)
        mode_values = forward_modes(grad_pre, spectral_weights[layer_index], forward_tables)
        if layer_index > 0:
            skip_term = jnp.einsum(
                "boxyz,oi->bixyz",
                grad_pre,
                skip_weights[layer_index],
                preferred_element_type=jnp.float32,
            )
            spectral = back_path(
                mode_values.astype(jnp.bfloat16), back_tables, rounded_product, to_bf16
            )
            incoming = skip_term + spectral
        else:
            folded = jnp.sum(mode_values * lift_weights[None, :, None, None, None], 1)[:, None]
            spectral = back_path(folded, back_tables, exact_product, keep_float)
            combined = jnp.sum(skip_weights[0].astype(jnp.float32) * lift_weights[None, :], 1)
            projected = jnp.sum(
                grad_pre.astype(jnp.float32) * combined[None, :, None, None, None], 1
            )
            perm_grad = projected + spectral[:, 0]
    return perm_grad


F32 = jnp.float32
BF16 = jnp.bfloat16
MESH = pl.DeviceIdType.MESH


class Plan:
    def __init__(self, mesh, channels):
        self.rows = mesh.shape["aa"]
        self.columns = mesh.shape["ba"]
        self.xb = NX // self.rows
        self.yb = NY // self.columns
        self.mb = KZ * KT // self.rows
        self.kb = KX // self.columns
        self.cells = NZ * NT
        self.spots = self.xb * self.yb
        self.channels = channels
        self.group = 4
        self.groups = channels // self.group
        self.tall = self.group * self.mb
        self.half = 128
        self.kmain = self.half // (2 * self.yb)
        self.width = 2 * self.kb * self.yb
        self.modes = self.kb * KY
        self.room = -(-self.modes // 128) * 128
        self.lines = self.mb * KY

    def fits(self):
        return (
            self.spots == self.half
            and self.half % self.yb == 0
            and self.yb % 16 == 0
            and self.half % (2 * self.yb) == 0
            and 2 * (self.width - self.half) == self.half
            and self.columns % 2 == 0
            and self.channels % self.group == 0
            and self.tall % 16 == 0
            and self.xb % 2 == 0
        )


def real_form(matrix):
    top = np.stack([matrix.real, matrix.imag], 1)
    low = np.stack([-matrix.imag, matrix.real], 1)
    return np.stack([top, low], 0)


def line_phase(count, length):
    turns = signed_freq(count)[:, None] * np.arange(length)[None, :] % length
    return np.exp(2j * math.pi * turns / length)


def dense_tables(plan):
    rows, columns = plan.rows, plan.columns
    eye_y = np.eye(plan.yb)
    eye_k = np.eye(plan.kb)
    along_x = line_phase(KX, NX)
    along_y = line_phase(KY, NY)
    plane_forward, plane_inverse = plane_tables()
    tables = {}

    def split(wide, axis):
        main, left = np.split(wide, [plan.kmain], axis + 1)
        shape = wide.shape[:axis] + (-1,) + wide.shape[axis + 4 :]
        return np.concatenate([main.reshape(shape), left.reshape(shape)], axis)

    tables["plane_in"] = plane_forward.transpose(1, 2, 0).reshape(2 * KZ * KT, plan.cells)
    part = real_form(along_x.conj().T).reshape(2, rows, plan.xb, 2, columns, plan.kb)
    wide = np.einsum("psxqgk,yw->spxygkqw", part, eye_y)
    wide = wide.reshape((rows * 2 * plan.spots,) + wide.shape[4:])
    tables["x_in"] = split(wide, 1)
    part = real_form(along_y.conj().T).reshape(2, columns, plan.yb, 2, KY)
    wide = split(np.einsum("pbyqj,kl->blpyqkj", part, eye_k), 0)
    wide = wide.reshape(columns * plan.width, 2, plan.modes)
    wide = np.pad(wide, ((0, 0), (0, 0), (0, plan.room - plan.modes)))
    tables["y_in"] = wide.reshape(columns * plan.width, 2 * plan.room)
    part = (real_form(along_y) / NY).reshape(2, KY, 2, columns, plan.yb)
    wide = split(np.einsum("pjqhy,kl->pkjhlqy", part, eye_k), 3)
    tables["y_out"] = wide.reshape(2, plan.modes, columns * plan.width)
    part = (real_form(along_x) / NX).reshape(2, columns, plan.kb, 2, rows, plan.xb)
    wide = split(np.einsum("pbkqnx,yw->bkpynqxw", part, eye_y), 0)
    tables["x_out"] = wide.reshape(columns * plan.width, rows * 2 * plan.spots)
    back = plane_inverse.reshape(2, rows, plan.mb, plan.cells).transpose(1, 0, 2, 3)
    tables["plane_out"] = back.reshape(2 * KZ * KT, plan.cells)
    return {name: jnp.asarray(table.astype(jnp.bfloat16)) for name, table in tables.items()}


def slope_twice(values):
    scaled = values * math.sqrt(0.5)
    bell = jnp.exp2(scaled * scaled * -math.log2(math.e))
    return 1.0 + lax.erf(scaled) + scaled * (2.0 / math.sqrt(math.pi)) * bell


def product(left, right, contract=((1,), (0,))):
    return lax.dot_general(left, right, (contract, ((), ())), preferred_element_type=F32)


def greet(plan):
    barrier = pltpu.get_barrier_semaphore()
    for axis, size in (("aa", plan.rows), ("ba", plan.columns)):
        for hop in range(1, size):
            peer = lax.rem(lax.axis_index(axis) + hop, size)
            pl.semaphore_signal(barrier, inc=1, device_id={axis: peer}, device_id_type=MESH)
    pl.semaphore_wait(barrier, plan.rows + plan.columns - 2)


class Tables:
    def __init__(self, sources, places, sems):
        self.sources, self.places, self.sems = sources, places, sems

    def copy(self, index):
        return pltpu.make_async_copy(self.sources[index], self.places[index], self.sems.at[index])

    def start(self):
        for index in range(len(self.sources)):
            self.copy(index).start()


class Exchange:
    def __init__(self, axis, size, out, into, sent, came):
        self.axis, self.size = axis, size
        self.out, self.into, self.sent, self.came = out, into, sent, came

    def copy(self, group, hop):
        me = lax.axis_index(self.axis)
        peer = lax.rem(me + hop, self.size)
        return pltpu.make_async_remote_copy(
            src_ref=self.out.at[group, peer],
            dst_ref=self.into.at[group, me],
            send_sem=self.sent.at[group, hop],
            recv_sem=self.came.at[group, hop],
            device_id={self.axis: peer},
            device_id_type=MESH,
        )

    def start(self, group):
        for hop in range(1, self.size):
            self.copy(group, hop).start()
        me = lax.axis_index(self.axis)
        self.into[group, me] = self.out[group, me]

    def arrive(self, group):
        for hop in range(1, self.size):
            self.copy(group, hop).wait_recv()

    def finish(self, groups):
        def drain(group, carry):
            for hop in range(1, self.size):
                self.copy(group, hop).wait_send()
            return carry

        lax.fori_loop(0, groups, drain, 0)


def exchange_scratch(plan, groups, tall):
    rows, columns = plan.rows, plan.columns
    return [
        pltpu.VMEM((groups, rows, tall, 2 * plan.spots), BF16),
        pltpu.VMEM((groups, rows, tall, 2 * plan.spots), BF16),
        pltpu.SemaphoreType.DMA((groups, rows)),
        pltpu.SemaphoreType.DMA((groups, rows)),
        pltpu.VMEM((groups, columns, tall + tall // 2, plan.half), BF16),
        pltpu.VMEM((groups, columns, tall + tall // 2, plan.half), BF16),
        pltpu.SemaphoreType.DMA((groups, columns)),
        pltpu.SemaphoreType.DMA((groups, columns)),
    ]


def exchanges(plan, scratch):
    return (
        Exchange("aa", plan.rows, *scratch[:4]),
        Exchange("ba", plan.columns, *scratch[4:8]),
    )


def plane_in(plan, group, wide, over_a):
    rows, mb, spots = plan.rows, plan.mb, plan.spots
    for owner in range(rows):
        halves = []
        for part in range(2):
            first = (part * rows + owner) * mb
            halves.append(
                jnp.concatenate(
                    [
                        wide[first : first + mb, c * spots : (c + 1) * spots]
                        for c in range(plan.group)
                    ],
                    0,
                )
            )
        over_a.out[group, owner] = jnp.concatenate(halves, 1).astype(BF16)
    over_a.start(group)


def joined(ref, group, size):
    return jnp.concatenate([ref[group, index] for index in range(size)], 1)


def low_lanes(rows, half):
    return lax.broadcasted_iota(jnp.int32, (rows, half), 1) < half // 2


def pack(plan, group, values, over_b):
    half = plan.half
    tall = values.shape[0]
    low = low_lanes(tall // 2, half)
    for pair in range(plan.columns // 2):
        first = (plan.columns + pair) * half
        left = values[:, first : first + half]
        turned = pltpu.roll(left, half // 2, 1)
        for side, (upper, lower) in enumerate(((left, turned), (turned, left))):
            owner = 2 * pair + side
            main = values[:, owner * half : (owner + 1) * half]
            rest = jnp.where(low, upper[: tall // 2], lower[tall // 2 :])
            over_b.out[group, owner] = jnp.concatenate([main, rest], 0).astype(BF16)
    over_b.start(group)


def unpack(plan, group, over_b):
    over_b.arrive(group)
    half = plan.half
    tall = over_b.into.shape[2] * 2 // 3
    low = low_lanes(tall // 2, half)
    mains = [over_b.into[group, index, :tall] for index in range(plan.columns)]
    for pair in range(plan.columns // 2):
        first, second = [over_b.into[group, 2 * pair + side, tall:].astype(F32) for side in (0, 1)]
        upper = jnp.where(low, first, pltpu.roll(second, half // 2, 1))
        lower = jnp.where(low, pltpu.roll(first, half // 2, 1), second)
        mains.append(jnp.concatenate([upper, lower], 0).astype(BF16))
    return jnp.concatenate(mains, 1)


def x_in(plan, group, table, over_a, over_b):
    over_a.arrive(group)
    result = product(joined(over_a.into, group, plan.rows), table[...])
    pack(plan, group, result, over_b)


def y_in(plan, group, table, over_b, sheet, real_first, imag_first):
    result = product(unpack(plan, group, over_b), table[...])
    mb = plan.mb
    for c in range(plan.group):
        for part in range(2):
            lane = part * plan.room
            row = (2 * c + part) * mb
            for half in range(plan.room // 128):
                first = lane + 128 * half
                piece = result[c * mb : (c + 1) * mb, first : first + 128]
                sheet[half, row : row + mb] = piece
    count = 2 * plan.group
    lines = []
    for m in range(mb):
        row = pl.ds(m, count, stride=mb)
        lines.append(jnp.concatenate([sheet[h, row, :] for h in range(plan.room // 128)], 1))
    for k in range(plan.kb):
        turned = jnp.concatenate([line[:, k * KY : (k + 1) * KY] for line in lines], 1)
        for c in range(plan.group):
            real = turned[2 * c : 2 * c + 1]
            imag = turned[2 * c + 1 : 2 * c + 2]
            real_first[c, k] = jnp.concatenate([real, imag], 0)
            imag_first[c, k] = jnp.concatenate([imag, -real], 0)


def mix_in(plan, weights, real_first, imag_first, real_sum, imag_sum):
    for c in range(plan.group):
        for k in range(plan.kb):
            first = real_first[c, k]
            second = imag_first[c, k]

            def add(i, carry):
                matrix = weights[0, c, i, k].astype(F32)
                real_sum[i, k] += matrix * first
                imag_sum[i, k] += matrix * second
                return carry

            lax.fori_loop(0, plan.channels, add, 0, unroll=10)


def fold_in(plan, group, weights, lift, folded):
    for c in range(plan.group):

        def line(k, carry):
            total = weights[0, c, 0, k].astype(F32) * lift[0]
            for i in range(1, plan.channels):
                total = total + weights[0, c, i, k].astype(F32) * lift[i]
            folded[group * plan.group + c, k] = total
            return carry

        lax.fori_loop(0, plan.kb, line, 0)


def by_row(plan, rows, sheet):
    count = rows[0].shape[0]
    for m in range(plan.mb):
        pieces = [row[:, m * KY : (m + 1) * KY] for row in rows]
        if plan.room > plan.modes:
            pieces.append(jnp.zeros((count, plan.room - plan.modes), F32))
        line = jnp.concatenate(pieces, 1)
        for half in range(plan.room // 128):
            row = pl.ds(m, count, stride=plan.mb)
            sheet[half, row, :] = line[:, half * 128 : (half + 1) * 128]


def sheet_rows(plan, sheet, first, last):
    halves = [sheet[half, first:last] for half in range(plan.room // 128)]
    return jnp.concatenate(halves, 1)[:, : plan.modes].astype(BF16)


def y_out(plan, group, parts, table, over_b):
    result = product(parts[0], table[0]) + product(parts[1], table[1])
    tall = over_b.out.shape[2] * 2 // 3
    if result.shape[0] < tall:
        more = jnp.zeros((tall - result.shape[0], result.shape[1]), F32)
        result = jnp.concatenate([result, more], 0)
    pack(plan, group, result, over_b)


def x_out(plan, group, table, over_b, over_a):
    values = unpack(plan, group, over_b)
    width = 2 * plan.spots
    for owner in range(plan.rows):
        cut = table[:, owner * width : (owner + 1) * width]
        over_a.out[group, owner] = product(values, cut).astype(BF16)
    over_a.start(group)


def plane_out(plan, group, count, over_a):
    over_a.arrive(group)
    mb, spots = plan.mb, plan.spots
    pieces = []
    for source in range(plan.rows):
        block = over_a.into[group, source].astype(F32)
        for part in range(2):
            pieces.append(
                jnp.concatenate(
                    [
                        block[c * mb : (c + 1) * mb, part * spots : (part + 1) * spots]
                        for c in range(count)
                    ],
                    1,
                )
            )
    return jnp.concatenate(pieces, 0).astype(BF16)


def forward_kernel(
    plan, cotangent, pre, weights, h_plane, h_x, h_y, weight, skip, modes,
    t_plane, t_x, t_y, table_sems, mix, field, wide, sheet, real_first, imag_first, real_sum, imag_sum, *scratch,
):
    step = pl.program_id(0)
    over_a, over_b = exchanges(plan, scratch)
    groups, group = plan.groups, plan.group
    lanes = 512
    tables = Tables((h_plane, h_x, h_y), (t_plane, t_x, t_y), table_sems)

    @pl.when(step == 0)
    def _():
        tables.start()
        greet(plan)
        real_sum[...] = jnp.zeros_like(real_sum)
        imag_sum[...] = jnp.zeros_like(imag_sum)

    @pl.when(step < groups)
    def _():
        def fields(c):
            for x in range(plan.xb):
                for first in range(0, plan.cells, lanes):
                    cut = pl.ds(first, lanes)
                    slope = slope_twice(pre[0, 0, c, x, :, cut].astype(F32))
                    value = cotangent[0, c, x, :, cut].astype(F32) * 0.5 * slope
                    field[step * group + c, x, :, cut] = value.astype(BF16)

        @pl.when(step == 0)
        def _():
            tables.copy(0).wait()

        for pair in range(0, group, 2):
            fields(pair)
            fields(pair + 1)
            values = field[pl.ds(step * group + pair, 2)].reshape(2 * plan.spots, plan.cells)
            lane = pl.ds(pair * plan.spots, 2 * plan.spots)
            wide[:, lane] = product(t_plane[...], values, ((1,), (1,)))
        plane_in(plan, step, wide, over_a)

    @pl.when(step == groups)
    def _():
        tile = plan.yb // 2
        wide_rows = plan.channels * tile
        row = lax.broadcasted_iota(jnp.int32, (wide_rows, plan.channels), 0)
        column = lax.broadcasted_iota(jnp.int32, (wide_rows, plan.channels), 1)
        spread = (row // tile == column).astype(F32).astype(BF16)
        tall = product(spread, weight[1], ((1,), (1,))).astype(BF16)
        full = product(tall, spread, ((1,), (1,)))
        row = lax.broadcasted_iota(jnp.int32, full.shape, 0)
        column = lax.broadcasted_iota(jnp.int32, full.shape, 1)
        mix[...] = jnp.where(row % tile == column % tile, full, 0.0).astype(BF16)

    @pl.when(step >= groups)
    def _():
        def line(index, carry):
            x = (step - groups) * (plan.xb // 2) + index
            tile = plan.yb // 2
            for first in range(0, plan.cells, lanes):
                cut = pl.ds(first, lanes)
                for y in (pl.ds(0, tile), pl.ds(tile, tile)):
                    values = field[:, x, y, cut].reshape(plan.channels * tile, lanes)
                    result = product(mix[...], values).astype(BF16)
                    skip[:, index, y, cut] = result.reshape(plan.channels, tile, lanes)
            return carry

        lax.fori_loop(0, plan.xb // 2, line, 0)

    @pl.when(step == 1)
    def _():
        tables.copy(1).wait()

    @pl.when(jnp.logical_and(step >= 1, step <= groups))
    def _():
        x_in(plan, step - 1, t_x, over_a, over_b)

    @pl.when(step == 2)
    def _():
        tables.copy(2).wait()

    @pl.when(step >= 2)
    def _():
        y_in(plan, step - 2, t_y, over_b, sheet, real_first, imag_first)
        mix_in(plan, weights, real_first, imag_first, real_sum, imag_sum)

    @pl.when(step == groups + 1)
    def _():
        def turn(index, carry):
            rows = []
            for k in range(plan.kb):
                row = []
                for total in (real_sum, imag_sum):
                    for c in range(group):
                        both = total[index * group + c, k]
                        row.append(both[:1] + both[1:])
                rows.append(jnp.concatenate(row, 0))
            by_row(plan, rows, sheet)
            modes[index] = sheet_rows(plan, sheet, 0, 2 * plan.tall)
            return carry

        lax.fori_loop(0, groups, turn, 0)
        over_a.finish(groups)
        over_b.finish(groups)


def middle_kernel(
    plan, modes, skip, pre, weights, weight, lift, lift_row, *refs,
):
    (h_s_y, h_s_x, h_s_plane, h_plane, h_x, h_y, result) = refs[:7]
    (s_y, s_x, s_plane, t_plane, t_x, t_y, table_sems) = refs[7:14]
    (lifted, packed, values, wide, field, sheet, real_first, imag_first) = refs[14:22]
    (folded, real_sum, imag_sum), scratch = refs[22:25], refs[25:]
    step = pl.program_id(0)
    back_a, back_b = exchanges(plan, scratch[:8])
    over_a, over_b = exchanges(plan, scratch[8:16])
    last_a, last_b = exchanges(plan, scratch[16:])
    groups, group, tall = plan.groups, plan.group, plan.tall
    lanes = 512
    sources = (h_s_y, h_s_x, h_s_plane, h_plane, h_x, h_y)
    tables = Tables(sources, (s_y, s_x, s_plane, t_plane, t_x, t_y), table_sems)

    @pl.when(step == 0)
    def _():
        tables.start()
        greet(plan)
        tables.copy(0).wait()

        def send(index, carry):
            y_out(plan, index, (modes[index, :tall], modes[index, tall:]), s_y, back_b)
            return carry

        lax.fori_loop(0, groups, send, 0)
        result[...] = jnp.zeros_like(result)
        combined = jnp.sum(weight[0].astype(F32) * lift_row[...], 1, keepdims=True)
        lifted[...] = jnp.broadcast_to(combined, lifted.shape)
        real_sum[...] = jnp.zeros_like(real_sum)
        imag_sum[...] = jnp.zeros_like(imag_sum)
        tables.copy(1).wait()

    def ahead(at, carry):
        x_out(plan, at, s_x, back_b, back_a)
        return carry

    first = jnp.where(step == 0, 0, jnp.minimum(step + 1, groups))
    lax.fori_loop(first, jnp.minimum(step + 2, groups), ahead, 0)

    @pl.when(step == 0)
    def _():
        for index in range(2, 6):
            tables.copy(index).wait()

    @pl.when(step < groups)
    def _():
        fold_in(plan, step, weights, lift, folded)
        at = step
        packed[...] = plane_out(plan, at, group, back_a)

        def spread(part):
            cut = pl.ds(part * lanes, lanes)
            values[:, cut] = product(packed[...], s_plane[:, cut], ((0,), (0,)))

        def fields(part):
            cut = pl.ds(part * lanes, lanes)
            for c in range(group):
                scale = lifted[pl.ds(at * group + c, 1), :]
                for x in range(plan.xb):
                    row = pl.ds((c * plan.xb + x) * plan.yb, plan.yb)
                    spot = pl.ds(x * plan.yb, plan.yb)
                    slope = 0.5 * slope_twice(pre[0, 0, c, x, :, cut].astype(F32))
                    incoming = values[row, cut] + skip[c, x, :, cut].astype(F32)
                    value = (incoming * slope).astype(BF16)
                    field[row, cut] = value
                    result[spot, cut] += value.astype(F32) * scale

        def gather(part):
            cut = pl.ds(2 * part * lanes, 2 * lanes)
            return product(t_plane[:, cut], field[:, cut], ((1,), (1,)))

        spread(0)
        spread(1)
        fields(0)
        spread(2)
        fields(1)
        wide[...] = gather(0)
        spread(3)
        fields(2)
        fields(3)
        wide[...] += gather(1)
        plane_in(plan, at, wide, over_a)

    @pl.when(jnp.logical_and(step >= 1, step <= groups))
    def _():
        x_in(plan, step - 1, t_x, over_a, over_b)

    @pl.when(step >= 2)
    def _():
        at = step - 2
        y_in(plan, at, t_y, over_b, sheet, real_first, imag_first)
        for c in range(group):
            matrix = folded[at * group + c]
            real_sum[...] += matrix * real_first[c]
            imag_sum[...] += matrix * imag_first[c]

    @pl.when(step == groups + 1)
    def _():
        rows = []
        for k in range(plan.kb):
            row = [total[k, :1] + total[k, 1:] for total in (real_sum, imag_sum)]
            rows.append(jnp.concatenate(row, 0))
        by_row(plan, rows, sheet)
        mb = plan.mb
        parts = [sheet_rows(plan, sheet, p * mb, (p + 1) * mb) for p in range(2)]
        y_out(plan, 0, parts, s_y, last_b)
        x_out(plan, 0, s_x, last_b, last_a)
        values_last = plane_out(plan, 0, 1, last_a)
        result[...] += product(values_last, s_plane[...], ((0,), (0,)))
        for each in (back_a, back_b, over_a, over_b):
            each.finish(groups)
        for each in (last_a, last_b):
            each.finish(1)


def whole():
    return pl.BlockSpec(memory_space=pltpu.VMEM, pipeline_mode=pl.Buffered(1))


VMEM_LIMIT = 62 * 1024 * 1024


def weight_spec(plan, layer, first):
    block = (1, plan.group, plan.channels, plan.kb, 2, plan.lines)
    last = plan.groups - 1
    return pl.BlockSpec(block, lambda s: (layer, jnp.clip(s - first, 0, last), 0, 0, 0, 0))


def table_scratch(tables, names):
    places = [pltpu.VMEM(tables[name].shape, BF16) for name in names]
    return places + [pltpu.SemaphoreType.DMA((len(names),))]


def mixing_scratch(plan):
    line = (2, plan.lines)
    return [
        pltpu.VMEM((plan.room // 128, 2 * plan.tall, 128), F32),
        pltpu.VMEM((plan.group, plan.kb) + line, F32),
        pltpu.VMEM((plan.group, plan.kb) + line, F32),
    ]


def forward_call(plan, layer, cotangent, pre_activations, weights, tables, skip_weights):
    groups, group = plan.groups, plan.group
    field = (plan.xb, plan.yb, plan.cells)
    sums = (plan.channels, plan.kb, 2, plan.lines)

    def at_group(step):
        return jnp.minimum(step, groups - 1)

    return pl.pallas_call(
        functools.partial(forward_kernel, plan),
        grid=(groups + 2,),
        in_specs=[
            pl.BlockSpec((1, group) + field, lambda s: (0, at_group(s), 0, 0, 0)),
            pl.BlockSpec((1, 1, group) + field, lambda s: (layer, 0, at_group(s), 0, 0, 0)),
            weight_spec(plan, layer, 2),
            pl.BlockSpec(memory_space=pl.ANY),
            pl.BlockSpec(memory_space=pl.ANY),
            pl.BlockSpec(memory_space=pl.ANY),
            whole(),
        ],
        out_specs=[
            pl.BlockSpec(
                (plan.channels, plan.xb // 2, plan.yb, plan.cells),
                lambda s: (0, jnp.clip(s - groups, 0, 1), 0, 0),
            ),
            pl.BlockSpec((groups, 2 * plan.tall, plan.modes), lambda s: (0, 0, 0)),
        ],
        out_shape=[
            jax.ShapeDtypeStruct((plan.channels,) + field, BF16),
            jax.ShapeDtypeStruct((groups, 2 * plan.tall, plan.modes), BF16),
        ],
        scratch_shapes=table_scratch(tables, ("plane_in", "x_in", "y_in"))
        + [
            pltpu.VMEM((plan.channels * plan.yb // 2,) * 2, BF16),
            pltpu.VMEM((plan.channels,) + field, BF16),
            pltpu.VMEM((2 * KZ * KT, group * plan.spots), F32),
        ]
        + mixing_scratch(plan)
        + [pltpu.VMEM(sums, F32), pltpu.VMEM(sums, F32)]
        + exchange_scratch(plan, groups, plan.tall),
        compiler_params=pltpu.CompilerParams(
            collective_id=1, has_side_effects=True, vmem_limit_bytes=VMEM_LIMIT
        ),
        name="forward",
    )(cotangent, pre_activations, weights, tables["plane_in"], tables["x_in"], tables["y_in"], skip_weights)


def middle_call(plan, layer, modes, skip, pre_activations, weights, weight, lift, tables):
    groups, group = plan.groups, plan.group
    field = (plan.xb, plan.yb, plan.cells)
    sums = (plan.kb, 2, plan.lines)

    def at_group(step):
        return jnp.minimum(step, groups - 1)

    names = ("y_out", "x_out", "plane_out", "plane_in", "x_in", "y_in")
    return pl.pallas_call(
        functools.partial(middle_kernel, plan),
        grid=(groups + 2,),
        in_specs=[
            whole(),
            pl.BlockSpec((group,) + field, lambda s: (at_group(s), 0, 0, 0)),
            pl.BlockSpec((1, 1, group) + field, lambda s: (layer, 0, at_group(s), 0, 0, 0)),
            weight_spec(plan, layer, 0),
            whole(),
            pl.BlockSpec(memory_space=pltpu.SMEM),
            whole(),
        ]
        + [pl.BlockSpec(memory_space=pl.ANY)] * len(names),
        out_specs=pl.BlockSpec((plan.spots, plan.cells), lambda s: (0, 0)),
        out_shape=jax.ShapeDtypeStruct((plan.spots, plan.cells), F32),
        scratch_shapes=table_scratch(tables, names)
        + [
            pltpu.VMEM((plan.channels, 512), F32),
            pltpu.VMEM((2 * KZ * KT, group * plan.spots), BF16),
            pltpu.VMEM((group * plan.spots, plan.cells), F32),
            pltpu.VMEM((2 * KZ * KT, group * plan.spots), F32),
            pltpu.VMEM((group * plan.spots, plan.cells), BF16),
        ]
        + mixing_scratch(plan)
        + [pltpu.VMEM((plan.channels,) + sums, F32)]
        + [pltpu.VMEM(sums, F32), pltpu.VMEM(sums, F32)]
        + exchange_scratch(plan, groups, plan.tall)
        + exchange_scratch(plan, groups, plan.tall)
        + exchange_scratch(plan, 1, -(-plan.mb // 16) * 16),
        compiler_params=pltpu.CompilerParams(
            collective_id=2, has_side_effects=True, vmem_limit_bytes=VMEM_LIMIT
        ),
        name="middle",
    )(
        modes, skip, pre_activations, weights, weight, lift, lift.reshape(1, -1),
        *[tables[name] for name in names],
    )


def per_device(plan, cotangent, pre_activations, spectral_weights, skip_weights, lift_weights):
    tables = dense_tables(plan)
    weights = spectral_weights.transpose(0, 2, 3, 4, 1, 5)
    skip, modes = forward_call(plan, 1, cotangent, pre_activations, weights, tables, skip_weights)
    result = middle_call(
        plan, 0, modes, skip, pre_activations, weights, skip_weights, lift_weights, tables
    )
    return result.reshape(1, plan.xb, plan.yb, plan.cells)


def solution(mesh):
    def step(cotangent, pre_activations, spectral_weights, skip_weights, lift_weights):
        plan = Plan(mesh, cotangent.shape[1])
        layers, samples = pre_activations.shape[:2]
        if layers == 2 and samples == 1 and plan.fits():
            body = functools.partial(per_device, plan)
        else:
            body = per_device_plain
        return body(cotangent, pre_activations, spectral_weights, skip_weights, lift_weights)

    return jax.shard_map(
        step,
        mesh=mesh,
        in_specs=(
            P(None, None, "aa", "ba", None),
            P(None, None, None, "aa", "ba", None),
            P(None, None, None, None, "ba", "aa"),
            P(),
            P(),
        ),
        out_specs=P(None, "aa", "ba", None),
        check_vma=False,
    )
```
